32 devices in a mesh: dp: 2 (over x), pz: 4 (over z), py: 4 (over y, core).
Axes of the slice: x: 2, y: 2, z: 4, core: 2. Of those that a mesh axis runs over, the one named last changes fastest.
Arguments:
- rho_re: float32 [64, 64, 64, 64], P('dp', None, 'py', 'pz'), parts along dimension 0
- rho_im: float32 [64, 64, 64, 64], P('dp', None, 'py', 'pz'), parts along dimension 0
- g_re: float32 [64, 64, 64], P('py', 'pz')
- g_im: float32 [64, 64, 64], P('py', 'pz')
Outputs:
- output 1: float32 [64, 64, 64, 64], P('dp', None, 'py', 'pz'), parts along dimension 0
- output 2: float32 [64, 64, 64, 64], P('dp', None, 'py', 'pz'), parts along dimension 0
- output 3: float32 [64, 64, 64, 64], P('dp', 'py', 'pz'), parts along dimension 0
- output 4: float32 [64, 64, 64, 64], P('dp', 'py', 'pz'), parts along dimension 0
There are 2 independent parts. The reference program is written for one: setup_inputs(seed, part) draws one part's arguments, and reference() takes and returns one part's arrays. A program takes and returns all parts, laid end to end along the dimension named above; an argument that names none is the same for every part.
All inputs are finite; a program needn't handle non-finite values.
Results may differ from the reference program's by a relative error of at most 0.001.
Values sent between devices are 32-bit elements.
A program may use at most 1 GiB of HBM per device.

```python
import jax
import jax.numpy as jnp
from jax import lax

GRID = 64
FIELDS = 32


def green_kernel():
    positions = jnp.arange(GRID)
    wavenum = jnp.where(positions < (GRID + 1) // 2, positions, positions - GRID).astype(jnp.float32)
    wave_sq = wavenum * wavenum * (16.0 / (GRID * GRID))
    return 1.0 / (1.0 + wave_sq[:, None, None] + 2.0 * wave_sq[None, :, None] + 3.0 * wave_sq[None, None, :])


def setup_inputs(seed: int = 0, part: int = 0) -> dict:
    part_key = jax.random.fold_in(jax.random.key(seed), part)
    key_re, key_im = jax.random.split(part_key)
    field_shape = (FIELDS, GRID, GRID, GRID)
    rho_re = jax.random.normal(key_re, field_shape, jnp.float32)
    rho_im = jax.random.normal(key_im, field_shape, jnp.float32)
    green_re_key, green_im_key = jax.random.split(jax.random.key(seed + 1))
    kernel = green_kernel()
    g_re = kernel * (1.0 + 0.5 * jax.random.normal(green_re_key, kernel.shape, jnp.float32))
    g_im = kernel * (0.5 * jax.random.normal(green_im_key, kernel.shape, jnp.float32))
    return {"rho_re": rho_re, "rho_im": rho_im, "g_re": g_re, "g_im": g_im}


def reference(rho_re, rho_im, g_re, g_im):
    green_fn = lax.complex(g_re, g_im)

    def one_field(field_pair):
        volume = lax.complex(field_pair[0], field_pair[1])
        spectrum = jnp.fft.fftn(volume, axes=(0, 1, 2), norm="ortho") * green_fn
        restored = jnp.fft.ifftn(spectrum, axes=(0, 1, 2), norm="ortho")
        return jnp.real(restored), jnp.imag(restored), jnp.real(spectrum), jnp.imag(spectrum)

    phi_re, phi_im, hat_re, hat_im = lax.map(one_field, (rho_re, rho_im))
    return (phi_re, phi_im, hat_re, hat_im)
```

```python
import functools

import jax
import jax.numpy as jnp
import numpy as np
from jax import lax
from jax.experimental import pallas as pl
from jax.experimental.pallas import tpu as pltpu
from jax.sharding import PartitionSpec as P

GRID = 64
SIDE = 4
BLOCK = 16
GROUP = 8
HALF = 8
HIGHEST = lax.Precision.HIGHEST
MESH = pl.DeviceIdType.MESH


def rotation(left, right, sign):
    angle = 2.0 * np.pi * (np.outer(left, right) % GRID) / GRID
    return np.cos(angle), sign * np.sin(angle)


def dft_matrix(rows_in, rows_out, sign, scale):
    cos, sin = rotation(rows_in, rows_out, sign)
    return np.block([[cos, sin], [-sin, cos]]) * scale


def tables():
    points = np.arange(GRID)
    kx = np.array([[[BLOCK * j + HALF * h + k for k in range(HALF)] for j in range(SIDE)] for h in range(2)])
    order = np.stack([kx, kx + GRID], axis=2).reshape(-1)
    first = dft_matrix(points, points, -1, 1.0 / 64).T[order]
    last = dft_matrix(points, points, 1, 1.0 / 8)[order]
    along_z = dft_matrix(points, points, -1, 1.0 / 8)
    back_z = dft_matrix(points, points, 1, 1.0 / 64)
    return [np.asarray(t, np.float32) for t in (first, along_z, back_z, last)]


def dft4(x):
    (a, b), (c, d), (e, f), (g, h) = x
    t0r, t0i, t1r, t1i = a + e, b + f, a - e, b - f
    t2r, t2i, t3r, t3i = c + g, d + h, c - g, d - h
    return [(t0r + t2r, t0i + t2i), (t1r + t3i, t1i - t3r), (t0r - t2r, t0i - t2i), (t1r - t3i, t1i + t3r)]


def dft8(x):
    r = np.float32(np.sqrt(0.5))
    even = [(x[i][0] + x[i + 4][0], x[i][1] + x[i + 4][1]) for i in range(4)]
    odd = [(x[i][0] - x[i + 4][0], x[i][1] - x[i + 4][1]) for i in range(4)]
    (p, q), (s, t), (u, v) = odd[1:]
    odd = [odd[0], ((p + q) * r, (q - p) * r), (t, -s), ((v - u) * r, -((u + v) * r))]
    out_even, out_odd = dft4(even), dft4(odd)
    return [out_even[0], out_odd[0], out_even[1], out_odd[1], out_even[2], out_odd[2], out_even[3], out_odd[3]]


def twiddle(value, power):
    re, im = value
    power %= GRID
    if power == 0:
        return value
    cos, sin = np.float32(np.cos(2 * np.pi * power / GRID)), np.float32(np.sin(2 * np.pi * power / GRID))
    return re * cos + im * sin, im * cos - re * sin


def dft64(src, dst, tmp, flip):
    first, second = (1, 0) if flip else (0, 1)
    for b in range(8):
        x = []
        for a in range(8):
            s, l = divmod(8 * a + b, BLOCK)
            x.append((src[s, l, first], src[s, l, second]))
        for k, value in enumerate(dft8(x)):
            re, im = twiddle(value, b * k)
            tmp[b, k, 0] = re
            tmp[b, k, 1] = im
    for k in range(8):
        out = dft8([(tmp[b, k, 0], tmp[b, k, 1]) for b in range(8)])
        for m, (re, im) in enumerate(out):
            s, l = divmod(k + 8 * m, BLOCK)
            dst[s, l, first] = re
            dst[s, l, second] = im


def block_transpose(x, lane):
    x = list(x)
    for bit in range(3):
        shift = BLOCK << bit
        low = (lane & shift) == 0
        for i in range(8):
            if i & (1 << bit) == 0:
                j = i | (1 << bit)
                a, b = x[i], x[j]
                x[i] = jnp.where(low, a, pltpu.roll(b, shift, 1))
                x[j] = jnp.where(low, pltpu.roll(a, 128 - shift, 1), b)
    return x


def kernel(rho_re, rho_im, g_re, g_im, w_first, w_z, w_back, w_last, phi, hat,
           in_re, in_im, sent, got, tmp, ga, gb, hat_stage, phi_stage,
           in_sem, hat_sem, phi_sem, own_sem, send_sem, recv_sem):
    fields = rho_re.shape[0]
    chunks = fields // GROUP
    units = 2 * chunks
    axis = ("py", "pz", "pz", "py")
    me = {name: lax.axis_index(name) for name in ("py", "pz")}

    barrier = pltpu.get_barrier_semaphore()
    for name in ("py", "pz"):
        for d in range(1, SIDE):
            pl.semaphore_signal(barrier, inc=1, device_id={name: lax.rem(me[name] + d, SIDE)}, device_id_type=MESH)

    def load(c):
        rows = pl.ds(c * GROUP, GROUP)
        return [pltpu.make_async_copy(rho.at[rows], buf.at[rows], in_sem.at[c, k])
                for k, (rho, buf) in enumerate(((rho_re, in_re), (rho_im, in_im)))]

    for c in range(chunks):
        for copy in load(c):
            copy.start()

    lane = lax.broadcasted_iota(jnp.int32, (8, 128), 1)

    def remote(phase, u, d):
        name = axis[phase]
        to = lax.rem(me[name] + d, SIDE)
        return pltpu.make_async_remote_copy(
            src_ref=sent.at[phase, u, to], dst_ref=got.at[phase, u, me[name]],
            send_sem=send_sem.at[phase, u, d - 1], recv_sem=recv_sem.at[phase, u, d - 1],
            device_id={name: to}, device_id_type=MESH)

    def own(phase, u):
        mine = me[axis[phase]]
        return pltpu.make_async_copy(sent.at[phase, u, mine], got.at[phase, u, mine], own_sem.at[phase, u])

    def send(phase, u):
        for d in (2, 1, 3) if axis[phase] == "pz" else (1, 3, 2):
            remote(phase, u, d).start()
        own(phase, u).start()

    def arrive(phase, u):
        for d in range(1, SIDE):
            remote(phase, u, d).wait_recv()
        own(phase, u).wait()

    def first_stage(c):
        for copy in load(c):
            copy.wait()

        def one(y, carry):
            rows = pl.ds(c * GROUP, GROUP)
            re = in_re[rows, y].reshape(GROUP * BLOCK, GRID)
            im = in_im[rows, y].reshape(GROUP * BLOCK, GRID)
            both = jnp.concatenate([re, im], axis=1)
            out = lax.dot_general(w_first[...], both, (((1,), (1,)), ((), ())), precision=HIGHEST,
                                  preferred_element_type=jnp.float32)
            out = out.reshape(2, SIDE, 2, HALF, 128)
            for h in range(2):
                for j in range(SIDE):
                    sent[0, 2 * c + h, j, y] = out[h, j]
            return carry

        lax.fori_loop(0, BLOCK, one, 0)

    def y_stage(u):
        arrive(0, u)
        dft64(got.at[0, u], sent.at[1, u], tmp, False)
        send(1, u)

    def hat_out(u):
        c, h = lax.div(u, 2), lax.rem(u, 2)
        return pltpu.make_async_copy(
            hat_stage.at[h],
            hat.at[pl.ds(c * GROUP, GROUP), pl.ds(h * (HALF * BLOCK), HALF * BLOCK)], hat_sem.at[h])

    STEP = 4

    def z_stage(u):
        h = lax.rem(u, 2)
        arrive(1, u)

        @pl.when(u >= 2)
        def _():
            hat_out(u - 2).wait()

        def one(step, carry):
            rows = []
            for i in range(STEP):
                ky = step * STEP + i
                rows += block_transpose([got[1, u, s, ky, c] for c in range(2) for s in range(SIDE)], lane)
            x = jnp.dot(jnp.concatenate(rows, axis=0), w_z[...], precision=HIGHEST,
                        preferred_element_type=jnp.float32)
            x = x.reshape(STEP, GROUP, HALF, 128)
            scaled = []
            for i in range(STEP):
                ky = step * STEP + i
                a, b = ga[h, ky], gb[h, ky]
                for f in range(GROUP):
                    v = x[i, f]
                    v = v * a + pltpu.roll(v, GRID, 1) * b
                    hat_stage[h, f, pl.ds(ky, HALF, stride=BLOCK), :] = v
                    scaled.append(v)
            x = jnp.dot(jnp.concatenate(scaled, axis=0), w_back[...], precision=HIGHEST,
                        preferred_element_type=jnp.float32)
            x = x.reshape(STEP, GROUP, HALF, 128)
            for i in range(STEP):
                ky = step * STEP + i
                out = block_transpose([x[i, f] for f in range(GROUP)], lane)
                for c in range(2):
                    for s in range(SIDE):
                        sent[2, u, s, ky, c] = out[c * SIDE + s]
            return carry

        lax.fori_loop(0, BLOCK // STEP, one, 0)
        send(2, u)
        hat_out(u).start()

    def back_y_stage(u):
        arrive(2, u)
        dft64(got.at[2, u], sent.at[3, u], tmp, True)
        send(3, u)

    def phi_out(c):
        slot = lax.rem(c, 2)
        return pltpu.make_async_copy(phi_stage.at[slot], phi.at[pl.ds(c * GROUP, GROUP)], phi_sem.at[slot])

    def last_stage(c):
        for h in range(2):
            arrive(3, 2 * c + h)
        slot = lax.rem(c, 2)

        @pl.when(c >= 2)
        def _():
            phi_out(c - 2).wait()

        def one(y, carry):
            x = jnp.concatenate([got[3, 2 * c + h, j, y].reshape(2 * HALF, 128)
                                 for h in range(2) for j in range(SIDE)], axis=0)
            out = lax.dot_general(x, w_last[...], (((0,), (0,)), ((), ())), precision=HIGHEST,
                                  preferred_element_type=jnp.float32)
            phi_stage[slot, :, pl.ds(pl.multiple_of(y * BLOCK, BLOCK), BLOCK), :] = out.reshape(GROUP, BLOCK, 128)
            return carry

        lax.fori_loop(0, BLOCK, one, 0)
        phi_out(c).start()

    for h in range(2):
        for ky in range(BLOCK):
            pick = pl.ds(h * HALF * BLOCK + ky, HALF, stride=BLOCK)
            re, im = g_re[pick, :], g_im[pick, :]
            ga[h, ky] = jnp.concatenate([re, re], axis=1)
            gb[h, ky] = jnp.concatenate([-im, im], axis=1)

    first_stage(0)
    pl.semaphore_wait(barrier, 2 * (SIDE - 1))
    send(0, 0)
    send(0, 1)

    def step(t, carry):
        @pl.when((lax.rem(t, 2) == 0) & (t // 2 + 1 < chunks))
        def _():
            c = lax.div(t, 2) + 1
            first_stage(c)
            send(0, 2 * c)
            send(0, 2 * c + 1)

        @pl.when(t < units)
        def _():
            y_stage(t)

        @pl.when((t >= 3) & (t < units + 3))
        def _():
            z_stage(t - 3)

        @pl.when((t >= 5) & (t < units + 5))
        def _():
            back_y_stage(t - 5)

        @pl.when((t >= 7) & (lax.rem(t, 2) == 1))
        def _():
            last_stage(lax.div(t - 7, 2))

        return carry

    lax.fori_loop(0, units + 6, step, 0)

    for u in range(units - 2, units):
        hat_out(u).wait()
    for c in range(chunks - 2, chunks):
        phi_out(c).wait()

    def finish(u, carry):
        for phase in range(4):
            for d in range(1, SIDE):
                remote(phase, u, d).wait_send()
        return carry

    lax.fori_loop(0, units, finish, 0)


def solve(rho_re, rho_im, g_re, g_im):
    fields = rho_re.shape[0]
    units = 2 * (fields // GROUP)
    f32 = jnp.float32
    vmem = pl.BlockSpec(memory_space=pltpu.VMEM)
    anywhere = pl.BlockSpec(memory_space=pl.ANY)
    weights = [jnp.asarray(t) for t in tables()]
    dma = pltpu.SemaphoreType.DMA
    phi, hat = pl.pallas_call(
        kernel,
        out_shape=[jax.ShapeDtypeStruct((fields, BLOCK * BLOCK, 128), f32)] * 2,
        in_specs=[anywhere] * 2 + [vmem] * 6,
        out_specs=[anywhere] * 2,
        scratch_shapes=[
            pltpu.VMEM((fields, BLOCK, BLOCK, GRID), f32),
            pltpu.VMEM((fields, BLOCK, BLOCK, GRID), f32),
            pltpu.VMEM((4, units, SIDE, BLOCK, 2, HALF, 128), f32),
            pltpu.VMEM((4, units, SIDE, BLOCK, 2, HALF, 128), f32),
            pltpu.VMEM((8, 8, 2, HALF, 128), f32),
            pltpu.VMEM((2, BLOCK, HALF, 128), f32),
            pltpu.VMEM((2, BLOCK, HALF, 128), f32),
            pltpu.VMEM((2, GROUP, HALF * BLOCK, 128), f32),
            pltpu.VMEM((2, GROUP, BLOCK * BLOCK, 128), f32),
            dma((fields // GROUP, 2)), dma((2,)), dma((2,)), dma((4, units)),
            dma((4, units, SIDE - 1)), dma((4, units, SIDE - 1)),
        ],
        compiler_params=pltpu.CompilerParams(collective_id=0, has_side_effects=True, vmem_limit_bytes=60 * 2**20),
        name="spectral_solve",
    )(jnp.transpose(rho_re, (0, 2, 3, 1)), jnp.transpose(rho_im, (0, 2, 3, 1)),
      g_re.reshape(BLOCK * BLOCK, GRID), g_im.reshape(BLOCK * BLOCK, GRID), *weights)
    phi = phi.reshape(fields, BLOCK, BLOCK, 128)
    hat = hat.reshape(fields, BLOCK, BLOCK, 128)
    phi_re = jnp.transpose(phi[..., :GRID], (0, 3, 1, 2))
    phi_im = jnp.transpose(phi[..., GRID:], (0, 3, 1, 2))
    return phi_re, phi_im, hat[..., :GRID], hat[..., GRID:]


def solution(mesh):
    space_layout = P("dp", None, "py", "pz")
    wave_layout = P("dp", "py", "pz", None)
    green_layout = P("py", "pz", None)
    return jax.shard_map(solve, mesh=mesh,
                         in_specs=(space_layout, space_layout, green_layout, green_layout),
                         out_specs=(space_layout, space_layout, wave_layout, wave_layout),
                         check_vma=False)
```

```python
import jax
import jax.numpy as jnp
import numpy as np
from jax import lax
from jax.experimental import pallas as pl
from jax.experimental.pallas import tpu as pltpu
from jax.sharding import PartitionSpec as P

GRID = 64
SIDE = 4
BLOCK = 16
GROUP = 8
HALF = 8
HIGHEST = lax.Precision.HIGHEST
MESH = pl.DeviceIdType.MESH


def rotation(left, right, sign):
    angle = 2.0 * np.pi * (np.outer(left, right) % GRID) / GRID
    return np.cos(angle), sign * np.sin(angle)


def dft_matrix(rows_in, rows_out, sign, scale):
    cos, sin = rotation(rows_in, rows_out, sign)
    return np.block([[cos, sin], [-sin, cos]]) * scale


def tables():
    points = np.arange(GRID)
    kx = np.array([[[BLOCK * j + HALF * h + k for k in range(HALF)] for j in range(SIDE)] for h in range(2)])
    order = np.stack([kx, kx + GRID], axis=2).reshape(-1)
    first = dft_matrix(points, points, -1, 1.0 / 64).T[order]
    last = dft_matrix(points, points, 1, 1.0 / 8)[order]
    along_z = dft_matrix(points, points, -1, 1.0 / 8)
    back_z = dft_matrix(points, points, 1, 1.0 / 64)
    return [np.asarray(t, np.float32) for t in (first, along_z, back_z, last)]


def dft4(x):
    (a, b), (c, d), (e, f), (g, h) = x
    t0r, t0i, t1r, t1i = a + e, b + f, a - e, b - f
    t2r, t2i, t3r, t3i = c + g, d + h, c - g, d - h
    return [(t0r + t2r, t0i + t2i), (t1r + t3i, t1i - t3r), (t0r - t2r, t0i - t2i), (t1r - t3i, t1i + t3r)]


def dft8(x):
    r = np.float32(np.sqrt(0.5))
    even = [(x[i][0] + x[i + 4][0], x[i][1] + x[i + 4][1]) for i in range(4)]
    odd = [(x[i][0] - x[i + 4][0], x[i][1] - x[i + 4][1]) for i in range(4)]
    (p, q), (s, t), (u, v) = odd[1:]
    odd = [odd[0], ((p + q) * r, (q - p) * r), (t, -s), ((v - u) * r, -((u + v) * r))]
    out_even, out_odd = dft4(even), dft4(odd)
    return [out_even[0], out_odd[0], out_even[1], out_odd[1], out_even[2], out_odd[2], out_even[3], out_odd[3]]


def twiddle(value, power):
    re, im = value
    power %= GRID
    if power == 0:
        return value
    cos, sin = np.float32(np.cos(2 * np.pi * power / GRID)), np.float32(np.sin(2 * np.pi * power / GRID))
    return re * cos + im * sin, im * cos - re * sin


def dft64(src, dst, tmp, flip):
    first, second = (1, 0) if flip else (0, 1)
    for b in range(8):
        x = []
        for a in range(8):
            s, l = divmod(8 * a + b, BLOCK)
            x.append((src[s, l, first], src[s, l, second]))
        for k, value in enumerate(dft8(x)):
            re, im = twiddle(value, b * k)
            tmp[b, k, 0] = re
            tmp[b, k, 1] = im
    for k in range(8):
        out = dft8([(tmp[b, k, 0], tmp[b, k, 1]) for b in range(8)])
        for m, (re, im) in enumerate(out):
            s, l = divmod(k + 8 * m, BLOCK)
            dst[s, l, first] = re
            dst[s, l, second] = im


def block_transpose(x, lane):
    x = list(x)
    for bit in range(3):
        shift = BLOCK << bit
        low = (lane & shift) == 0
        for i in range(8):
            if i & (1 << bit) == 0:
                j = i | (1 << bit)
                a, b = x[i], x[j]
                x[i] = jnp.where(low, a, pltpu.roll(b, shift, 1))
                x[j] = jnp.where(low, pltpu.roll(a, 128 - shift, 1), b)
    return x


def kernel(rho_re, rho_im, g_re, g_im, w_first, w_z, w_back, w_last, phi_re, phi_im, hat_re, hat_im, last,
           in_re, in_im, sent, got, tmp, gv_re, gv_im, ga, gb, v_first, v_z, v_back, v_last,
           in_sem, small_sem, own_sem, send_sem, recv_sem):
    fields = rho_re.shape[0]
    chunks = fields // GROUP
    units = 2 * chunks
    axis = ("py", "pz", "pz", "py")
    me = {name: lax.axis_index(name) for name in ("py", "pz")}

    def load(c):
        rows = pl.ds(c * GROUP, GROUP)
        return [pltpu.make_async_copy(rho.at[rows], buf.at[rows], in_sem.at[c, k])
                for k, (rho, buf) in enumerate(((rho_re, in_re), (rho_im, in_im)))]

    small = [pltpu.make_async_copy(src, dst, small_sem.at[k]) for k, (src, dst) in enumerate(
        ((w_first, v_first), (w_z, v_z), (w_back, v_back), (w_last, v_last), (g_re, gv_re), (g_im, gv_im)))]

    small[0].start()
    for copy in load(0):
        copy.start()
    barrier = pltpu.get_barrier_semaphore()
    for name in ("py", "pz"):
        for d in range(1, SIDE):
            pl.semaphore_signal(barrier, inc=1, device_id={name: lax.rem(me[name] + d, SIDE)}, device_id_type=MESH)

    lane = lax.broadcasted_iota(jnp.int32, (8, 128), 1)

    def target(phase, u, slot):
        return last.at[u, slot] if phase == 3 else got.at[phase, u, slot]

    def remote(phase, u, d, part=None):
        name = axis[phase]
        to = lax.rem(me[name] + d, SIDE)
        src, dst = sent.at[phase, u, to], target(phase, u, me[name])
        if part is not None:
            src, dst = src.at[part], dst.at[part]
        return pltpu.make_async_remote_copy(
            src_ref=src, dst_ref=dst, send_sem=send_sem.at[phase, u, d - 1], recv_sem=recv_sem.at[phase, u, d - 1],
            device_id={name: to}, device_id_type=MESH)

    def own(phase, u):
        mine = me[axis[phase]]
        return pltpu.make_async_copy(sent.at[phase, u, mine], target(phase, u, mine), own_sem.at[phase, u])

    def send(phase, u):
        for d in (2, 1, 3) if axis[phase] == "pz" else (1, 3, 2):
            remote(phase, u, d).start()
        own(phase, u).start()

    def arrive(phase, u):
        for d in range(1, SIDE):
            remote(phase, u, d).wait_recv()
        own(phase, u).wait()

    def x_rows(c, part):
        def one(i, carry):
            for k in range(X_STEP):
                y = part * QUARTER + i * X_STEP + k
                rows = pl.ds(c * GROUP, GROUP)
                re = in_re[rows, y].reshape(GROUP * BLOCK, GRID)
                im = in_im[rows, y].reshape(GROUP * BLOCK, GRID)
                both = jnp.concatenate([re, im], axis=1)
                out = lax.dot_general(v_first[...], both, (((1,), (1,)), ((), ())), precision=HIGHEST,
                                      preferred_element_type=jnp.float32)
                out = out.reshape(2, SIDE, 2, HALF, 128)
                for h in range(2):
                    for j in range(SIDE):
                        sent[0, 2 * c + h, j, y] = out[h, j]
            return carry

        lax.fori_loop(0, QUARTER // X_STEP, one, 0)

    def first_stage(c):
        for copy in load(c):
            copy.wait()

        def quarter(part, carry):
            x_rows(c, part)
            for d in (1, 3, 2):
                remote(0, 2 * c, d, pl.ds(part * QUARTER, QUARTER)).start()
            return carry

        lax.fori_loop(0, BLOCK // QUARTER, quarter, 0)
        own(0, 2 * c).start()
        send(0, 2 * c + 1)

    def y_stage(u):
        arrive(0, u)
        dft64(got.at[0, u], sent.at[1, u], tmp, False)
        send(1, u)

    def z_stage(u):
        c, h = lax.div(u, 2), lax.rem(u, 2)
        arrive(1, u)

        def one(step, carry):
            rows = []
            for i in range(Z_STEP):
                ky = step * Z_STEP + i
                rows += block_transpose([got[1, u, s, ky, c] for c in range(2) for s in range(SIDE)], lane)
            x = jnp.dot(jnp.concatenate(rows, axis=0), v_z[...], precision=HIGHEST,
                        preferred_element_type=jnp.float32)
            x = x.reshape(Z_STEP, GROUP, HALF, 128)
            scaled = []
            for i in range(Z_STEP):
                ky = step * Z_STEP + i
                a, b = ga[h, ky], gb[h, ky]
                for f in range(GROUP):
                    v = x[i, f]
                    v = v * a + pltpu.roll(v, GRID, 1) * b
                    place = pl.ds(h * (HALF * BLOCK) + ky, HALF, stride=BLOCK)
                    hat_re[c * GROUP + f, place, :] = v[:, :GRID]
                    hat_im[c * GROUP + f, place, :] = pltpu.roll(v, GRID, 1)[:, :GRID]
                    scaled.append(v)
            x = jnp.dot(jnp.concatenate(scaled, axis=0), v_back[...], precision=HIGHEST,
                        preferred_element_type=jnp.float32)
            x = x.reshape(Z_STEP, GROUP, HALF, 128)
            for i in range(Z_STEP):
                ky = step * Z_STEP + i
                out = block_transpose([x[i, f] for f in range(GROUP)], lane)
                for part in range(2):
                    for s in range(SIDE):
                        sent[2, u, s, ky, part] = out[part * SIDE + s]
            return carry

        lax.fori_loop(0, BLOCK // Z_STEP, one, 0)
        send(2, u)

    def back_y_stage(u):
        arrive(2, u)
        dft64(got.at[2, u], sent.at[3, u], tmp, True)
        send(3, u)

    def last_stage(c):
        for h in range(2):
            arrive(3, 2 * c + h)
        back_x(last, 2 * c, v_last, phi_re, phi_im, c * GROUP)

    first = small[0]
    first.wait()
    pl.semaphore_wait(barrier, 2 * (SIDE - 1))
    first_stage(0)
    for c in range(1, chunks):
        for copy in load(c):
            copy.start()
    for copy in small[1:]:
        copy.start()
    for copy in small[1:]:
        copy.wait()

    def spread(ky, carry):
        for h in range(2):
            pick = pl.ds(h * HALF * BLOCK + ky, HALF, stride=BLOCK)
            re, im = gv_re[pick, :], gv_im[pick, :]
            ga[h, ky] = jnp.concatenate([re, re], axis=1)
            gb[h, ky] = jnp.concatenate([-im, im], axis=1)
        return carry

    lax.fori_loop(0, BLOCK, spread, 0)

    def step(t, carry):
        @pl.when((lax.rem(t, 2) == 0) & (t // 2 + 1 < chunks))
        def _():
            first_stage(lax.div(t, 2) + 1)

        @pl.when(t < units)
        def _():
            y_stage(t)

        @pl.when((t >= 3) & (t < units + 3))
        def _():
            z_stage(t - 3)

        @pl.when((t >= 5) & (t < units + 5))
        def _():
            back_y_stage(t - 5)

        @pl.when((t >= 7) & (lax.rem(t, 2) == 1))
        def _():
            last_stage(lax.div(t - 7, 2))

        return carry

    lax.fori_loop(0, units + 5, step, 0)
    for h in range(2):
        arrive(3, units - 2 + h)

    def finish(u, carry):
        for phase in range(4):
            for d in range(1, SIDE):
                remote(phase, u, d).wait_send()
        return carry

    lax.fori_loop(0, units, finish, 0)


def back_x(src, unit, table, out_re, out_im, start):
    def one(i, carry):
        for k in range(X_STEP):
            y = i * X_STEP + k
            x = jnp.concatenate([src[unit + h, j, y].reshape(2 * HALF, 128)
                                 for h in range(2) for j in range(SIDE)], axis=0)
            out = lax.dot_general(x, table[...], (((0,), (0,)), ((), ())), precision=HIGHEST,
                                  preferred_element_type=jnp.float32)
            place = pl.ds(pl.multiple_of(y * BLOCK, BLOCK), BLOCK)
            where = pl.ds(start, GROUP)
            out_re[where, place, :] = out[:, :GRID].reshape(GROUP, BLOCK, GRID)
            out_im[where, place, :] = pltpu.roll(out, GRID, 1)[:, :GRID].reshape(GROUP, BLOCK, GRID)
        return carry

    lax.fori_loop(0, BLOCK // X_STEP, one, 0)


def write_out(phi_re, phi_im, hat_re, hat_im, last, table, out_phi_re, out_phi_im, out_hat_re, out_hat_im,
              re, im, sem):
    done = phi_re.shape[0]
    copies = [pltpu.make_async_copy(src, dst, sem.at[k]) for k, (src, dst) in enumerate((
        (hat_re, out_hat_re), (hat_im, out_hat_im), (phi_re, out_phi_re.at[pl.ds(0, done)]),
        (phi_im, out_phi_im.at[pl.ds(0, done)])))]
    for copy in copies:
        copy.start()
    back_x(last, last.shape[0] - 2, table, re, im, 0)
    for k, (src, dst) in enumerate(((re, out_phi_re), (im, out_phi_im))):
        copies.append(pltpu.make_async_copy(src, dst.at[pl.ds(done, GROUP)], sem.at[4 + k]))
        copies[-1].start()
    for copy in copies:
        copy.wait()


QUARTER = 4
X_STEP = 2
Z_STEP = 4


def solve(rho_re, rho_im, g_re, g_im):
    fields = rho_re.shape[0]
    chunks = fields // GROUP
    units = 2 * chunks
    f32 = jnp.float32
    vmem = pl.BlockSpec(memory_space=pltpu.VMEM)
    anywhere = pl.BlockSpec(memory_space=pl.ANY)
    weights = [jnp.asarray(t) for t in tables()]
    dma = pltpu.SemaphoreType.DMA
    flat = BLOCK * BLOCK
    square = pltpu.VMEM((128, 128), f32)
    held = pl.pallas_call(
        kernel,
        out_shape=[pltpu.VMEM((fields - GROUP, flat, GRID), f32)] * 2 + [pltpu.VMEM((fields, flat, GRID), f32)] * 2
        + [pltpu.VMEM((units, SIDE, BLOCK, 2, HALF, 128), f32)],
        in_specs=[anywhere] * 8,
        out_specs=[vmem] * 5,
        scratch_shapes=[
            pltpu.VMEM((fields, BLOCK, BLOCK, GRID), f32),
            pltpu.VMEM((fields, BLOCK, BLOCK, GRID), f32),
            pltpu.VMEM((4, units, SIDE, BLOCK, 2, HALF, 128), f32),
            pltpu.VMEM((3, units, SIDE, BLOCK, 2, HALF, 128), f32),
            pltpu.VMEM((8, 8, 2, HALF, 128), f32),
            pltpu.VMEM((flat, GRID), f32),
            pltpu.VMEM((flat, GRID), f32),
            pltpu.VMEM((2, BLOCK, HALF, 128), f32),
            pltpu.VMEM((2, BLOCK, HALF, 128), f32),
            square, square, square, square,
            dma((chunks, 2)), dma((6,)), dma((4, units)),
            dma((4, units, SIDE - 1)), dma((4, units, SIDE - 1)),
        ],
        compiler_params=pltpu.CompilerParams(collective_id=0, has_side_effects=True, vmem_limit_bytes=41 * 2**20),
        name="spectral_solve",
    )(jnp.transpose(rho_re, (0, 2, 3, 1)), jnp.transpose(rho_im, (0, 2, 3, 1)),
      g_re.reshape(flat, GRID), g_im.reshape(flat, GRID), *weights)
    held = [pltpu.with_memory_space_constraint(x, pltpu.VMEM) for x in held]
    phi_re, phi_im, hat_re, hat_im = pl.pallas_call(
        write_out,
        out_shape=[jax.ShapeDtypeStruct((fields, flat, GRID), f32)] * 4,
        in_specs=[vmem] * 6,
        out_specs=[anywhere] * 4,
        scratch_shapes=[pltpu.VMEM((GROUP, flat, GRID), f32), pltpu.VMEM((GROUP, flat, GRID), f32), dma((6,))],
        compiler_params=pltpu.CompilerParams(vmem_limit_bytes=6 * 2**20),
        name="write_out",
    )(*held, weights[3])
    shape = (fields, BLOCK, BLOCK, GRID)
    phi_re = jnp.transpose(phi_re.reshape(shape), (0, 3, 1, 2))
    phi_im = jnp.transpose(phi_im.reshape(shape), (0, 3, 1, 2))
    return phi_re, phi_im, hat_re.reshape(shape), hat_im.reshape(shape)


def solution(mesh):
    space_layout = P("dp", None, "py", "pz")
    wave_layout = P("dp", "py", "pz", None)
    green_layout = P("py", "pz", None)
    return jax.shard_map(solve, mesh=mesh,
                         in_specs=(space_layout, space_layout, green_layout, green_layout),
                         out_specs=(space_layout, space_layout, wave_layout, wave_layout),
                         check_vma=False)
```

```python
import jax
import jax.numpy as jnp
import numpy as np
from jax import lax
from jax.experimental import pallas as pl
from jax.experimental.pallas import tpu as pltpu
from jax.sharding import PartitionSpec as P

GRID = 64
SIDE = 4
BLOCK = 16
GROUP = 8
HALF = 8
QUAD = 4
HIGHEST = lax.Precision.HIGHEST
MESH = pl.DeviceIdType.MESH


def rotation(left, right, sign):
    angle = 2.0 * np.pi * (np.outer(left, right) % GRID) / GRID
    return np.cos(angle), sign * np.sin(angle)


def dft_matrix(rows_in, rows_out, sign, scale):
    cos, sin = rotation(rows_in, rows_out, sign)
    return np.block([[cos, sin], [-sin, cos]]) * scale


def tables():
    points = np.arange(GRID)
    kx = np.array([[[BLOCK * j + QUAD * q + k for k in range(QUAD)] for j in range(SIDE)] for q in range(QUAD)])
    order = np.stack([kx, kx + GRID], axis=2).reshape(-1)
    first = dft_matrix(points, points, -1, 1.0 / 64).T[order]
    last = dft_matrix(points, points, 1, 1.0 / 8)[order]
    along_z = dft_matrix(points, points, -1, 1.0 / 8)
    back_z = dft_matrix(points, points, 1, 1.0 / 64)
    return [np.asarray(t, np.float32) for t in (first, along_z, back_z, last)]


def dft4(x, turn):
    even, odd = x[0] + x[2], x[0] - x[2]
    both, side = x[1] + x[3], turn(x[1] - x[3])
    return [even + both, odd + side, even - both, odd - side]


def dft8(x, turn):
    r = np.float32(np.sqrt(0.5))
    even = [x[i] + x[i + 4] for i in range(4)]
    odd = [x[i] - x[i + 4] for i in range(4)]
    odd = [odd[0], (odd[1] + turn(odd[1])) * r, turn(odd[2]), (turn(odd[3]) - odd[3]) * r]
    even, odd = dft4(even, turn), dft4(odd, turn)
    return [value for pair in zip(even, odd) for value in pair]


def dft64(src, dst, tmp, sign):
    row = lax.broadcasted_iota(jnp.int32, (8, 128), 0)
    signs = jnp.where(row < QUAD, np.float32(-sign), np.float32(sign))

    def turn(value):
        return pltpu.roll(value, QUAD, 0) * signs

    def twiddle(value, power):
        if power == 0:
            return value
        angle = 2 * np.pi * power / GRID
        return value * np.float32(np.cos(angle)) + turn(value) * np.float32(np.sin(angle))

    for b in range(8):
        x = [src[divmod(8 * a + b, BLOCK)] for a in range(8)]
        for k, value in enumerate(dft8(x, turn)):
            tmp[b, k] = twiddle(value, b * k)
    for k in range(8):
        out = dft8([tmp[b, k] for b in range(8)], turn)
        for m, value in enumerate(out):
            dst[divmod(k + 8 * m, BLOCK)] = value


def block_transpose(x, lane):
    x = list(x)
    for bit in range(3):
        shift = BLOCK << bit
        low = (lane & shift) == 0
        for i in range(8):
            if i & (1 << bit) == 0:
                j = i | (1 << bit)
                a, b = x[i], x[j]
                x[i] = jnp.where(low, a, pltpu.roll(b, shift, 1))
                x[j] = jnp.where(low, pltpu.roll(a, 128 - shift, 1), b)
    return x


def kernel(rho_re, rho_im, g_re, g_im, w_first, w_z, w_back, w_last, phi_re, phi_im, hat_re, hat_im, last,
           in_re, in_im, sent, got, tmp, gv_re, gv_im, ga, gb, v_first, v_z, v_back, v_last,
           in_sem, small_sem, own_sem, send_sem, recv_sem):
    fields = rho_re.shape[0]
    chunks = fields // GROUP
    units = QUAD * chunks
    axis = ("py", "pz", "pz", "py")
    me = {name: lax.axis_index(name) for name in ("py", "pz")}

    def load(c):
        rows = pl.ds(c * GROUP, GROUP)
        return [pltpu.make_async_copy(rho.at[rows], buf.at[rows], in_sem.at[c, k])
                for k, (rho, buf) in enumerate(((rho_re, in_re), (rho_im, in_im)))]

    small = [pltpu.make_async_copy(src, dst, small_sem.at[k]) for k, (src, dst) in enumerate(
        ((w_first, v_first), (w_z, v_z), (w_back, v_back), (w_last, v_last), (g_re, gv_re), (g_im, gv_im)))]

    small[0].start()
    for copy in load(0):
        copy.start()
    barrier = pltpu.get_barrier_semaphore()
    for name in ("py", "pz"):
        for d in range(1, SIDE):
            pl.semaphore_signal(barrier, inc=1, device_id={name: lax.rem(me[name] + d, SIDE)}, device_id_type=MESH)

    lane = lax.broadcasted_iota(jnp.int32, (8, 128), 1)
    top = lax.broadcasted_iota(jnp.int32, (8, 128), 0) < QUAD

    def swap(a, b):
        return jnp.where(top, a, pltpu.roll(b, QUAD, 0)), jnp.where(top, pltpu.roll(a, QUAD, 0), b)

    def target(phase, u, slot):
        return last.at[u, slot] if phase == 3 else got.at[phase, u, slot]

    def remote(phase, u, d, part=None):
        name = axis[phase]
        to = lax.rem(me[name] + d, SIDE)
        src, dst = sent.at[phase, u, to], target(phase, u, me[name])
        if part is not None:
            src, dst = src.at[part], dst.at[part]
        return pltpu.make_async_remote_copy(
            src_ref=src, dst_ref=dst, send_sem=send_sem.at[phase, u, d - 1], recv_sem=recv_sem.at[phase, u, d - 1],
            device_id={name: to}, device_id_type=MESH)

    def own(phase, u):
        mine = me[axis[phase]]
        return pltpu.make_async_copy(sent.at[phase, u, mine], target(phase, u, mine), own_sem.at[phase, u])

    def send(phase, u):
        for d in (2, 1, 3) if axis[phase] == "pz" else (1, 3, 2):
            remote(phase, u, d).start()
        own(phase, u).start()

    def arrive(phase, u):
        for d in range(1, SIDE):
            remote(phase, u, d).wait_recv()
        own(phase, u).wait()

    def x_rows(c, part):
        def one(i, carry):
            for k in range(X_STEP):
                y = part * QUARTER + i * X_STEP + k
                rows = pl.ds(c * GROUP, GROUP)
                re = in_re[rows, y].reshape(GROUP * BLOCK, GRID)
                im = in_im[rows, y].reshape(GROUP * BLOCK, GRID)
                both = jnp.concatenate([re, im], axis=1)
                out = lax.dot_general(v_first[...], both, (((1,), (1,)), ((), ())), precision=HIGHEST,
                                      preferred_element_type=jnp.float32)
                out = out.reshape(QUAD, SIDE, 2 * QUAD, 128)
                for q in range(QUAD):
                    for j in range(SIDE):
                        sent[0, QUAD * c + q, j, y] = out[q, j]
            return carry

        lax.fori_loop(0, QUARTER // X_STEP, one, 0)

    def first_stage(c):
        def quarter(part, carry):
            x_rows(c, part)
            for d in (1, 3, 2):
                remote(0, QUAD * c, d, pl.ds(part * QUARTER, QUARTER)).start()
            return carry

        lax.fori_loop(0, BLOCK // QUARTER, quarter, 0)
        own(0, QUAD * c).start()
        for q in range(1, QUAD):
            send(0, QUAD * c + q)

    def y_stage(u):
        arrive(0, u)
        dft64(got.at[0, u], sent.at[1, u], tmp, -1)
        send(1, u)

    def z_stage(u):
        c, h = lax.div(u, 2), lax.rem(u, 2)
        for q in range(2):
            arrive(1, 2 * u + q)

        def one(step, carry):
            rows = []
            for i in range(Z_STEP):
                ky = step * Z_STEP + i
                parts = [swap(got[1, 2 * u, s, ky], got[1, 2 * u + 1, s, ky]) for s in range(SIDE)]
                rows += block_transpose([part[k] for k in range(2) for part in parts], lane)
            x = jnp.dot(jnp.concatenate(rows, axis=0), v_z[...], precision=HIGHEST,
                        preferred_element_type=jnp.float32)
            x = x.reshape(Z_STEP, GROUP, HALF, 128)
            scaled = []
            for i in range(Z_STEP):
                ky = step * Z_STEP + i
                a, b = ga[h, ky], gb[h, ky]
                for f in range(GROUP):
                    v = x[i, f]
                    v = v * a + pltpu.roll(v, GRID, 1) * b
                    place = pl.ds(h * (HALF * BLOCK) + ky, HALF, stride=BLOCK)
                    hat_re[c * GROUP + f, place, :] = v[:, :GRID]
                    hat_im[c * GROUP + f, place, :] = pltpu.roll(v, GRID, 1)[:, :GRID]
                    scaled.append(v)
            x = jnp.dot(jnp.concatenate(scaled, axis=0), v_back[...], precision=HIGHEST,
                        preferred_element_type=jnp.float32)
            x = x.reshape(Z_STEP, GROUP, HALF, 128)
            for i in range(Z_STEP):
                ky = step * Z_STEP + i
                out = block_transpose([x[i, f] for f in range(GROUP)], lane)
                for s in range(SIDE):
                    sent[2, 2 * u, s, ky], sent[2, 2 * u + 1, s, ky] = swap(out[s], out[SIDE + s])
            return carry

        lax.fori_loop(0, BLOCK // Z_STEP, one, 0)
        for q in range(2):
            send(2, 2 * u + q)

    def back_y_stage(u):
        arrive(2, u)
        dft64(got.at[2, u], sent.at[3, u], tmp, 1)
        send(3, u)

    def last_stage(c):
        for q in range(QUAD):
            arrive(3, QUAD * c + q)
        back_x(last, QUAD * c, v_last, phi_re, phi_im, c * GROUP)

    small[0].wait()
    for copy in load(0):
        copy.wait()
    for c in range(1, chunks):
        for copy in load(c):
            copy.start()
    for copy in small[1:]:
        copy.start()
    pl.semaphore_wait(barrier, 2 * (SIDE - 1))
    first_stage(0)
    for copy in small[1:]:
        copy.wait()

    def spread(ky, carry):
        for h in range(2):
            pick = pl.ds(h * HALF * BLOCK + ky, HALF, stride=BLOCK)
            re, im = gv_re[pick, :], gv_im[pick, :]
            ga[h, ky] = jnp.concatenate([re, re], axis=1)
            gb[h, ky] = jnp.concatenate([-im, im], axis=1)
        return carry

    lax.fori_loop(0, BLOCK, spread, 0)

    pairs = units // 2

    def step(t, carry):
        @pl.when(t < pairs)
        def _():
            lax.fori_loop(2 * t, 2 * t + 2, lambda u, k: (y_stage(u), k)[1], 0)

        @pl.when((lax.rem(t, 2) == 0) & (t // 2 + 1 < chunks))
        def _():
            c = lax.div(t, 2) + 1
            for copy in load(c):
                copy.wait()
            first_stage(c)

        @pl.when((t >= 3) & (t < pairs + 3))
        def _():
            z_stage(t - 3)

        @pl.when((t >= 5) & (t < pairs + 5))
        def _():
            lax.fori_loop(2 * (t - 5), 2 * (t - 5) + 2, lambda u, k: (back_y_stage(u), k)[1], 0)

        @pl.when((t >= 7) & (lax.rem(t, 2) == 1))
        def _():
            last_stage(lax.div(t - 7, 2))

        return carry

    lax.fori_loop(0, pairs + 5, step, 0)
    for q in range(QUAD):
        arrive(3, units - QUAD + q)

    def finish(u, carry):
        for phase in range(4):
            for d in range(1, SIDE):
                remote(phase, u, d).wait_send()
        return carry

    lax.fori_loop(0, units, finish, 0)


def back_x(src, unit, table, out_re, out_im, start):
    def one(i, carry):
        for k in range(X_STEP):
            y = i * X_STEP + k
            x = jnp.concatenate([src[unit + q, j, y] for q in range(QUAD) for j in range(SIDE)], axis=0)
            out = lax.dot_general(x, table[...], (((0,), (0,)), ((), ())), precision=HIGHEST,
                                  preferred_element_type=jnp.float32)
            place = pl.ds(pl.multiple_of(y * BLOCK, BLOCK), BLOCK)
            where = pl.ds(start, GROUP)
            out_re[where, place, :] = out[:, :GRID].reshape(GROUP, BLOCK, GRID)
            out_im[where, place, :] = pltpu.roll(out, GRID, 1)[:, :GRID].reshape(GROUP, BLOCK, GRID)
        return carry

    lax.fori_loop(0, BLOCK // X_STEP, one, 0)


def write_out(phi_re, phi_im, hat_re, hat_im, last, table, out_phi_re, out_phi_im, out_hat_re, out_hat_im,
              re, im, sem):
    done = phi_re.shape[0]
    copies = [pltpu.make_async_copy(src, dst, sem.at[k]) for k, (src, dst) in enumerate((
        (hat_re, out_hat_re), (hat_im, out_hat_im), (phi_re, out_phi_re.at[pl.ds(0, done)]),
        (phi_im, out_phi_im.at[pl.ds(0, done)])))]
    for copy in copies:
        copy.start()
    back_x(last, last.shape[0] - QUAD, table, re, im, 0)
    for k, (src, dst) in enumerate(((re, out_phi_re), (im, out_phi_im))):
        copies.append(pltpu.make_async_copy(src, dst.at[pl.ds(done, GROUP)], sem.at[4 + k]))
        copies[-1].start()
    for copy in copies:
        copy.wait()


QUARTER = 4
X_STEP = 4
Z_STEP = 4


def solve(rho_re, rho_im, g_re, g_im):
    fields = rho_re.shape[0]
    chunks = fields // GROUP
    units = QUAD * chunks
    f32 = jnp.float32
    vmem = pl.BlockSpec(memory_space=pltpu.VMEM)
    anywhere = pl.BlockSpec(memory_space=pl.ANY)
    weights = [jnp.asarray(t) for t in tables()]
    dma = pltpu.SemaphoreType.DMA
    flat = BLOCK * BLOCK
    square = pltpu.VMEM((128, 128), f32)
    held = pl.pallas_call(
        kernel,
        out_shape=[pltpu.VMEM((fields - GROUP, flat, GRID), f32)] * 2 + [pltpu.VMEM((fields, flat, GRID), f32)] * 2
        + [pltpu.VMEM((units, SIDE, BLOCK, 2 * QUAD, 128), f32)],
        in_specs=[anywhere] * 8,
        out_specs=[vmem] * 5,
        scratch_shapes=[
            pltpu.VMEM((fields, BLOCK, BLOCK, GRID), f32),
            pltpu.VMEM((fields, BLOCK, BLOCK, GRID), f32),
            pltpu.VMEM((4, units, SIDE, BLOCK, 2 * QUAD, 128), f32),
            pltpu.VMEM((3, units, SIDE, BLOCK, 2 * QUAD, 128), f32),
            pltpu.VMEM((8, 8, 2 * QUAD, 128), f32),
            pltpu.VMEM((flat, GRID), f32),
            pltpu.VMEM((flat, GRID), f32),
            pltpu.VMEM((2, BLOCK, HALF, 128), f32),
            pltpu.VMEM((2, BLOCK, HALF, 128), f32),
            square, square, square, square,
            dma((chunks, 2)), dma((6,)), dma((4, units)),
            dma((4, units, SIDE - 1)), dma((4, units, SIDE - 1)),
        ],
        compiler_params=pltpu.CompilerParams(collective_id=0, has_side_effects=True, vmem_limit_bytes=41 * 2**20),
        name="spectral_solve",
    )(jnp.transpose(rho_re, (0, 2, 3, 1)), jnp.transpose(rho_im, (0, 2, 3, 1)),
      g_re.reshape(flat, GRID), g_im.reshape(flat, GRID), *weights)
    held = [pltpu.with_memory_space_constraint(x, pltpu.VMEM) for x in held]
    phi_re, phi_im, hat_re, hat_im = pl.pallas_call(
        write_out,
        out_shape=[jax.ShapeDtypeStruct((fields, flat, GRID), f32)] * 4,
        in_specs=[vmem] * 6,
        out_specs=[anywhere] * 4,
        scratch_shapes=[pltpu.VMEM((GROUP, flat, GRID), f32), pltpu.VMEM((GROUP, flat, GRID), f32), dma((6,))],
        compiler_params=pltpu.CompilerParams(vmem_limit_bytes=6 * 2**20),
        name="write_out",
    )(*held, weights[3])
    shape = (fields, BLOCK, BLOCK, GRID)
    phi_re = jnp.transpose(phi_re.reshape(shape), (0, 3, 1, 2))
    phi_im = jnp.transpose(phi_im.reshape(shape), (0, 3, 1, 2))
    return phi_re, phi_im, hat_re.reshape(shape), hat_im.reshape(shape)


def solution(mesh):
    space_layout = P("dp", None, "py", "pz")
    wave_layout = P("dp", "py", "pz", None)
    green_layout = P("py", "pz", None)
    return jax.shard_map(solve, mesh=mesh,
                         in_specs=(space_layout, space_layout, green_layout, green_layout),
                         out_specs=(space_layout, space_layout, wave_layout, wave_layout),
                         check_vma=False)
```

```python
import jax
import jax.numpy as jnp
import numpy as np
from jax import lax
from jax.experimental import pallas as pl
from jax.experimental.pallas import tpu as pltpu
from jax.sharding import PartitionSpec as P

GRID = 64
SIDE = 4
BLOCK = 16
GROUP = 8
HALF = 8
QUAD = 4
HIGHEST = lax.Precision.HIGHEST
MESH = pl.DeviceIdType.MESH


def rotation(left, right, sign):
    angle = 2.0 * np.pi * (np.outer(left, right) % GRID) / GRID
    return np.cos(angle), sign * np.sin(angle)


def dft_matrix(rows_in, rows_out, sign, scale):
    cos, sin = rotation(rows_in, rows_out, sign)
    return np.block([[cos, sin], [-sin, cos]]) * scale


def tables():
    points = np.arange(GRID)
    kx = np.array([[[BLOCK * j + QUAD * q + k for k in range(QUAD)] for j in range(SIDE)] for q in range(QUAD)])
    order = np.stack([kx, kx + GRID], axis=2).reshape(-1)
    first = dft_matrix(points, points, -1, 1.0 / 64).T[order]
    last = dft_matrix(points, points, 1, 1.0 / 8)[order]
    along_z = dft_matrix(points, points, -1, 1.0 / 8)
    back_z = dft_matrix(points, points, 1, 1.0 / 64)
    return [np.asarray(t, np.float32) for t in (first, along_z, back_z, last)]


def dft4(x, turn):
    even, odd = x[0] + x[2], x[0] - x[2]
    both, side = x[1] + x[3], turn(x[1] - x[3])
    return [even + both, odd + side, even - both, odd - side]


def dft8(x, turn):
    r = np.float32(np.sqrt(0.5))
    even = [x[i] + x[i + 4] for i in range(4)]
    odd = [x[i] - x[i + 4] for i in range(4)]
    odd = [odd[0], (odd[1] + turn(odd[1])) * r, turn(odd[2]), (turn(odd[3]) - odd[3]) * r]
    even, odd = dft4(even, turn), dft4(odd, turn)
    return [value for pair in zip(even, odd) for value in pair]


def dft64(src, dst, tmp, sign):
    row = lax.broadcasted_iota(jnp.int32, (8, 128), 0)
    signs = jnp.where(row < QUAD, np.float32(-sign), np.float32(sign))

    def turn(value):
        return pltpu.roll(value, QUAD, 0) * signs

    def twiddle(value, power):
        if power == 0:
            return value
        angle = 2 * np.pi * power / GRID
        return value * np.float32(np.cos(angle)) + turn(value) * np.float32(np.sin(angle))

    for b in range(8):
        x = [src[divmod(8 * a + b, BLOCK)] for a in range(8)]
        for k, value in enumerate(dft8(x, turn)):
            tmp[b, k] = twiddle(value, b * k)
    for k in range(8):
        out = dft8([tmp[b, k] for b in range(8)], turn)
        for m, value in enumerate(out):
            dst[divmod(k + 8 * m, BLOCK)] = value


def block_transpose(x, lane):
    x = list(x)
    for bit in range(3):
        shift = BLOCK << bit
        low = (lane & shift) == 0
        for i in range(8):
            if i & (1 << bit) == 0:
                j = i | (1 << bit)
                a, b = x[i], x[j]
                x[i] = jnp.where(low, a, pltpu.roll(b, shift, 1))
                x[j] = jnp.where(low, pltpu.roll(a, 128 - shift, 1), b)
    return x


def kernel(rho_re, rho_im, g_re, g_im, w_first, w_z, w_back, w_last, phi_re, phi_im, hat_re, hat_im, last,
           in_re, in_im, sent, got, tmp, gv_re, gv_im, ga, gb, v_first, v_z, v_back, v_last,
           part_sem, in_sem, small_sem, own_sem, send_sem, recv_sem):
    fields = rho_re.shape[0]
    chunks = fields // GROUP
    units = QUAD * chunks
    axis = ("py", "pz", "pz", "py")
    me = {name: lax.axis_index(name) for name in ("py", "pz")}

    barrier = pltpu.get_barrier_semaphore()
    for name in ("py", "pz"):
        for d in range(1, SIDE):
            pl.semaphore_signal(barrier, inc=1, device_id={name: lax.rem(me[name] + d, SIDE)}, device_id_type=MESH)

    def load_part(part):
        where = pl.ds(0, GROUP), pl.ds(part * QUARTER, QUARTER)
        return [pltpu.make_async_copy(rho.at[where], buf.at[where], part_sem.at[part, k])
                for k, (rho, buf) in enumerate(((rho_re, in_re), (rho_im, in_im)))]

    def load(c):
        rows = pl.ds(c * GROUP, GROUP)
        return [pltpu.make_async_copy(rho.at[rows], buf.at[rows], in_sem.at[c, k])
                for k, (rho, buf) in enumerate(((rho_re, in_re), (rho_im, in_im)))]

    small = [pltpu.make_async_copy(src, dst, small_sem.at[k]) for k, (src, dst) in enumerate(
        ((w_first, v_first), (w_z, v_z), (w_back, v_back), (w_last, v_last), (g_re, gv_re), (g_im, gv_im)))]

    small[0].start()
    for part in range(BLOCK // QUARTER):
        for copy in load_part(part):
            copy.start()
    lane = lax.broadcasted_iota(jnp.int32, (8, 128), 1)
    top = lax.broadcasted_iota(jnp.int32, (8, 128), 0) < QUAD

    def swap(a, b):
        return jnp.where(top, a, pltpu.roll(b, QUAD, 0)), jnp.where(top, pltpu.roll(a, QUAD, 0), b)

    def target(phase, u, slot):
        return last.at[u, slot] if phase == 3 else got.at[phase, u, slot]

    def remote(phase, u, d, part=None):
        name = axis[phase]
        to = lax.rem(me[name] + d, SIDE)
        src, dst = sent.at[phase, u, to], target(phase, u, me[name])
        if part is not None:
            src, dst = src.at[part], dst.at[part]
        return pltpu.make_async_remote_copy(
            src_ref=src, dst_ref=dst, send_sem=send_sem.at[phase, u, d - 1], recv_sem=recv_sem.at[phase, u, d - 1],
            device_id={name: to}, device_id_type=MESH)

    def own(phase, u):
        mine = me[axis[phase]]
        return pltpu.make_async_copy(sent.at[phase, u, mine], target(phase, u, mine), own_sem.at[phase, u])

    def send(phase, u):
        for d in (2, 1, 3) if axis[phase] == "pz" else (1, 3, 2):
            remote(phase, u, d).start()
        own(phase, u).start()

    def arrive(phase, u):
        for d in range(1, SIDE):
            remote(phase, u, d).wait_recv()
        own(phase, u).wait()

    def x_rows(c, part):
        def one(i, carry):
            rows = pl.ds(c * GROUP, GROUP)
            start = part * QUARTER + i * X_STEP
            both = []
            for k in range(X_STEP):
                re = in_re[rows, start + k].reshape(GROUP * BLOCK, GRID)
                im = in_im[rows, start + k].reshape(GROUP * BLOCK, GRID)
                both.append(jnp.concatenate([re, im], axis=1))
            out = lax.dot_general(v_first[...], jnp.concatenate(both, axis=0), (((1,), (1,)), ((), ())),
                                  precision=HIGHEST, preferred_element_type=jnp.float32)
            out = out.reshape(QUAD, SIDE, 2 * QUAD, X_STEP * 128)
            for k in range(X_STEP):
                for q in range(QUAD):
                    for j in range(SIDE):
                        sent[0, QUAD * c + q, j, start + k] = out[q, j, :, k * 128:(k + 1) * 128]
            return carry

        lax.fori_loop(0, QUARTER // X_STEP, one, 0)

    def send_part(part):
        for d in (1, 3, 2):
            remote(0, 0, d, pl.ds(part * QUARTER, QUARTER)).start()

    def first_stage(c):
        lax.fori_loop(0, BLOCK // QUARTER, lambda part, k: (x_rows(c, part), k)[1], 0)
        for q in range(QUAD):
            send(0, QUAD * c + q)

    def opening():
        def quarter(part, carry):
            for copy in load_part(part):
                copy.wait()
            x_rows(0, part)

            @pl.when(part == 1)
            def _():
                pl.semaphore_wait(barrier, 2 * (SIDE - 1))
                send_part(0)

            @pl.when(part >= 1)
            def _():
                send_part(part)

            return carry

        lax.fori_loop(0, BLOCK // QUARTER, quarter, 0)
        own(0, 0).start()
        for q in range(1, QUAD):
            send(0, q)

    def y_stage(u):
        arrive(0, u)
        dft64(got.at[0, u], sent.at[1, u], tmp, -1)
        send(1, u)

    def z_stage(u):
        c, h = lax.div(u, 2), lax.rem(u, 2)
        for q in range(2):
            arrive(1, 2 * u + q)

        def one(step, carry):
            rows = []
            for i in range(Z_STEP):
                ky = step * Z_STEP + i
                parts = [swap(got[1, 2 * u, s, ky], got[1, 2 * u + 1, s, ky]) for s in range(SIDE)]
                rows += block_transpose([part[k] for k in range(2) for part in parts], lane)
            x = jnp.dot(jnp.concatenate(rows, axis=0), v_z[...], precision=HIGHEST,
                        preferred_element_type=jnp.float32)
            x = x.reshape(Z_STEP, GROUP, HALF, 128)
            scaled = []
            for i in range(Z_STEP):
                ky = step * Z_STEP + i
                a, b = ga[h, ky], gb[h, ky]
                for f in range(GROUP):
                    v = x[i, f]
                    v = v * a + pltpu.roll(v, GRID, 1) * b
                    place = pl.ds(h * (HALF * BLOCK) + ky, HALF, stride=BLOCK)
                    hat_re[c * GROUP + f, place, :] = v[:, :GRID]
                    hat_im[c * GROUP + f, place, :] = pltpu.roll(v, GRID, 1)[:, :GRID]
                    scaled.append(v)
            x = jnp.dot(jnp.concatenate(scaled, axis=0), v_back[...], precision=HIGHEST,
                        preferred_element_type=jnp.float32)
            x = x.reshape(Z_STEP, GROUP, HALF, 128)
            for i in range(Z_STEP):
                ky = step * Z_STEP + i
                out = block_transpose([x[i, f] for f in range(GROUP)], lane)
                for s in range(SIDE):
                    sent[2, 2 * u, s, ky], sent[2, 2 * u + 1, s, ky] = swap(out[s], out[SIDE + s])
            return carry

        lax.fori_loop(0, BLOCK // Z_STEP, one, 0)
        for q in range(2):
            send(2, 2 * u + q)

    def back_y_stage(u):
        arrive(2, u)
        dft64(got.at[2, u], sent.at[3, u], tmp, 1)
        send(3, u)

    def last_stage(c):
        for q in range(QUAD):
            arrive(3, QUAD * c + q)
        back_x(last, QUAD * c, v_last, phi_re, phi_im, c * GROUP)

    for c in range(1, chunks):
        for copy in load(c):
            copy.start()
    for copy in small[1:]:
        copy.start()
    small[0].wait()
    opening()
    for copy in small[1:]:
        copy.wait()

    def spread(ky, carry):
        for h in range(2):
            pick = pl.ds(h * HALF * BLOCK + ky, HALF, stride=BLOCK)
            re, im = gv_re[pick, :], gv_im[pick, :]
            ga[h, ky] = jnp.concatenate([re, re], axis=1)
            gb[h, ky] = jnp.concatenate([-im, im], axis=1)
        return carry

    lax.fori_loop(0, BLOCK, spread, 0)

    pairs = units // 2

    def step(t, carry):
        @pl.when(t < pairs)
        def _():
            lax.fori_loop(2 * t, 2 * t + 2, lambda u, k: (y_stage(u), k)[1], 0)

        @pl.when((lax.rem(t, 2) == 0) & (t // 2 + 1 < chunks))
        def _():
            c = lax.div(t, 2) + 1
            for copy in load(c):
                copy.wait()
            first_stage(c)

        @pl.when((t >= 3) & (t < pairs + 3))
        def _():
            z_stage(t - 3)

        @pl.when(t >= LAG)
        def _():
            lax.fori_loop(2 * (t - LAG), 2 * (t - LAG) + 2, lambda u, k: (back_y_stage(u), k)[1], 0)

        @pl.when((t >= LAG + 2) & (lax.rem(t - LAG, 2) == 0))
        def _():
            last_stage(lax.div(t - LAG, 2) - 1)

        return carry

    lax.fori_loop(0, pairs + LAG, step, 0)

    def sent_all(phase, first, end):
        def one(u, carry):
            for d in range(1, SIDE):
                remote(phase, u, d).wait_send()
            return carry

        lax.fori_loop(first, end, one, 0)

    for phase in range(3):
        sent_all(phase, 0, units)
    sent_all(3, 0, units - 2)
    for q in range(QUAD):
        arrive(3, units - QUAD + q)
    sent_all(3, units - 2, units)


def back_x(src, unit, table, out_re, out_im, start):
    def one(i, carry):
        x = [jnp.concatenate([src[unit + q, j, i * X_STEP + k] for q in range(QUAD) for j in range(SIDE)], axis=0)
             for k in range(X_STEP)]
        out = lax.dot_general(jnp.concatenate(x, axis=1), table[...], (((0,), (0,)), ((), ())), precision=HIGHEST,
                              preferred_element_type=jnp.float32)
        where = pl.ds(start, GROUP)
        for k in range(X_STEP):
            place = pl.ds(pl.multiple_of((i * X_STEP + k) * BLOCK, BLOCK), BLOCK)
            part = out[k * 128:(k + 1) * 128]
            out_re[where, place, :] = part[:, :GRID].reshape(GROUP, BLOCK, GRID)
            out_im[where, place, :] = pltpu.roll(part, GRID, 1)[:, :GRID].reshape(GROUP, BLOCK, GRID)
        return carry

    lax.fori_loop(0, BLOCK // X_STEP, one, 0)


def write_out(phi_re, phi_im, hat_re, hat_im, last, table, out_phi_re, out_phi_im, out_hat_re, out_hat_im,
              re, im, sem):
    done = phi_re.shape[0]
    copies = [pltpu.make_async_copy(src, dst, sem.at[k]) for k, (src, dst) in enumerate((
        (hat_re, out_hat_re), (hat_im, out_hat_im), (phi_re, out_phi_re.at[pl.ds(0, done)]),
        (phi_im, out_phi_im.at[pl.ds(0, done)])))]
    for copy in copies:
        copy.start()
    back_x(last, last.shape[0] - QUAD, table, re, im, 0)
    for k, (src, dst) in enumerate(((re, out_phi_re), (im, out_phi_im))):
        copies.append(pltpu.make_async_copy(src, dst.at[pl.ds(done, GROUP)], sem.at[4 + k]))
        copies[-1].start()
    for copy in copies:
        copy.wait()


QUARTER = 4
LAG = 6
X_STEP = 4
Z_STEP = 4


def solve(rho_re, rho_im, g_re, g_im):
    fields = rho_re.shape[0]
    chunks = fields // GROUP
    units = QUAD * chunks
    f32 = jnp.float32
    vmem = pl.BlockSpec(memory_space=pltpu.VMEM)
    anywhere = pl.BlockSpec(memory_space=pl.ANY)
    weights = [jnp.asarray(t) for t in tables()]
    dma = pltpu.SemaphoreType.DMA
    flat = BLOCK * BLOCK
    square = pltpu.VMEM((128, 128), f32)
    held = pl.pallas_call(
        kernel,
        out_shape=[pltpu.VMEM((fields - GROUP, flat, GRID), f32)] * 2 + [pltpu.VMEM((fields, flat, GRID), f32)] * 2
        + [pltpu.VMEM((units, SIDE, BLOCK, 2 * QUAD, 128), f32)],
        in_specs=[anywhere] * 8,
        out_specs=[vmem] * 5,
        scratch_shapes=[
            pltpu.VMEM((fields, BLOCK, BLOCK, GRID), f32),
            pltpu.VMEM((fields, BLOCK, BLOCK, GRID), f32),
            pltpu.VMEM((4, units, SIDE, BLOCK, 2 * QUAD, 128), f32),
            pltpu.VMEM((3, units, SIDE, BLOCK, 2 * QUAD, 128), f32),
            pltpu.VMEM((8, 8, 2 * QUAD, 128), f32),
            pltpu.VMEM((flat, GRID), f32),
            pltpu.VMEM((flat, GRID), f32),
            pltpu.VMEM((2, BLOCK, HALF, 128), f32),
            pltpu.VMEM((2, BLOCK, HALF, 128), f32),
            square, square, square, square,
            dma((BLOCK // QUARTER, 2)), dma((chunks, 2)), dma((6,)), dma((4, units)),
            dma((4, units, SIDE - 1)), dma((4, units, SIDE - 1)),
        ],
        compiler_params=pltpu.CompilerParams(collective_id=0, has_side_effects=True, vmem_limit_bytes=41 * 2**20),
        name="spectral_solve",
    )(jnp.transpose(rho_re, (0, 2, 3, 1)), jnp.transpose(rho_im, (0, 2, 3, 1)),
      g_re.reshape(flat, GRID), g_im.reshape(flat, GRID), *weights)
    held = [pltpu.with_memory_space_constraint(x, pltpu.VMEM) for x in held]
    phi_re, phi_im, hat_re, hat_im = pl.pallas_call(
        write_out,
        out_shape=[jax.ShapeDtypeStruct((fields, flat, GRID), f32)] * 4,
        in_specs=[vmem] * 6,
        out_specs=[anywhere] * 4,
        scratch_shapes=[pltpu.VMEM((GROUP, flat, GRID), f32), pltpu.VMEM((GROUP, flat, GRID), f32), dma((6,))],
        compiler_params=pltpu.CompilerParams(vmem_limit_bytes=6 * 2**20),
        name="write_out",
    )(*held, weights[3])
    shape = (fields, BLOCK, BLOCK, GRID)
    phi_re = jnp.transpose(phi_re.reshape(shape), (0, 3, 1, 2))
    phi_im = jnp.transpose(phi_im.reshape(shape), (0, 3, 1, 2))
    return phi_re, phi_im, hat_re.reshape(shape), hat_im.reshape(shape)


def solution(mesh):
    space_layout = P("dp", None, "py", "pz")
    wave_layout = P("dp", "py", "pz", None)
    green_layout = P("py", "pz", None)
    return jax.shard_map(solve, mesh=mesh,
                         in_specs=(space_layout, space_layout, green_layout, green_layout),
                         out_specs=(space_layout, space_layout, wave_layout, wave_layout),
                         check_vma=False)
```

```python
import jax
import jax.numpy as jnp
import numpy as np
from jax import lax
from jax.experimental import pallas as pl
from jax.experimental.pallas import tpu as pltpu
from jax.sharding import PartitionSpec as P

GRID = 64
SIDE = 4
BLOCK = 16
GROUP = 8
HALF = 8
QUAD = 4
PAIR = 2
HIGHEST = lax.Precision.HIGHEST
MESH = pl.DeviceIdType.MESH


def rotation(left, right, sign):
    angle = 2.0 * np.pi * (np.outer(left, right) % GRID) / GRID
    return np.cos(angle), sign * np.sin(angle)


def dft_matrix(rows_in, rows_out, sign, scale):
    cos, sin = rotation(rows_in, rows_out, sign)
    return np.block([[cos, sin], [-sin, cos]]) * scale


def tables():
    points = np.arange(GRID)
    q, j, h, c, k = np.ix_(range(QUAD), range(SIDE), range(2), range(2), range(PAIR))
    order = (BLOCK * j + HALF * (q // 2) + PAIR * (q % 2) + QUAD * h + k + GRID * c).reshape(-1)
    first = dft_matrix(points, points, -1, 1.0 / 64).T[order]
    last = dft_matrix(points, points, 1, 1.0 / 8)[order]
    along_z = dft_matrix(points, points, -1, 1.0 / 8)
    back_z = dft_matrix(points, points, 1, 1.0 / 64)
    return [np.asarray(t, np.float32) for t in (first, along_z, back_z, last)]


def dft4(x, turn):
    even, odd = x[0] + x[2], x[0] - x[2]
    both, side = x[1] + x[3], turn(x[1] - x[3])
    return [even + both, odd + side, even - both, odd - side]


def dft8(x, turn):
    r = np.float32(np.sqrt(0.5))
    even = [x[i] + x[i + 4] for i in range(4)]
    odd = [x[i] - x[i + 4] for i in range(4)]
    odd = [odd[0], (odd[1] + turn(odd[1])) * r, turn(odd[2]), (turn(odd[3]) - odd[3]) * r]
    even, odd = dft4(even, turn), dft4(odd, turn)
    return [value for pair in zip(even, odd) for value in pair]


def real_rows():
    return (lax.broadcasted_iota(jnp.int32, (8, 128), 0) & PAIR) == 0


def dft64(src, dst, tmp, sign):
    real = real_rows()
    signs = jnp.where(real, np.float32(-sign), np.float32(sign))

    def turn(value):
        return jnp.where(real, pltpu.roll(value, 8 - PAIR, 0), pltpu.roll(value, PAIR, 0)) * signs

    def twiddle(value, power):
        if power == 0:
            return value
        angle = 2 * np.pi * power / GRID
        return value * np.float32(np.cos(angle)) + turn(value) * np.float32(np.sin(angle))

    for b in range(8):
        x = [src[divmod(8 * a + b, BLOCK)] for a in range(8)]
        for k, value in enumerate(dft8(x, turn)):
            tmp[b, k] = twiddle(value, b * k)
    for k in range(8):
        out = dft8([tmp[b, k] for b in range(8)], turn)
        for m, value in enumerate(out):
            dst[divmod(k + 8 * m, BLOCK)] = value


def block_transpose(x, lane):
    x = list(x)
    for bit in range(3):
        shift = BLOCK << bit
        low = (lane & shift) == 0
        for i in range(8):
            if i & (1 << bit) == 0:
                j = i | (1 << bit)
                a, b = x[i], x[j]
                x[i] = jnp.where(low, a, pltpu.roll(b, shift, 1))
                x[j] = jnp.where(low, pltpu.roll(a, 128 - shift, 1), b)
    return x


def kernel(rho_re, rho_im, g_re, g_im, w_first, w_z, w_back, w_last, phi_re, phi_im, hat_re, hat_im, last,
           in_re, in_im, sent, got, half_got, half_sent, tmp, gv_re, gv_im, ga, gb, v_first, v_z, v_back, v_last,
           part_sem, in_sem, small_sem, own_sem, send_sem, recv_sem,
           half_own_sem, half_send_sem, half_recv_sem):
    fields = rho_re.shape[0]
    chunks = fields // GROUP
    units = QUAD * chunks
    axis = ("py", "pz", "pz", "py")
    me = {name: lax.axis_index(name) for name in ("py", "pz")}

    barrier = pltpu.get_barrier_semaphore()
    for name in ("py", "pz"):
        for d in range(1, SIDE):
            pl.semaphore_signal(barrier, inc=1, device_id={name: lax.rem(me[name] + d, SIDE)}, device_id_type=MESH)

    def load_part(part):
        where = pl.ds(0, GROUP), pl.ds(part * QUARTER, QUARTER)
        return [pltpu.make_async_copy(rho.at[where], buf.at[where], part_sem.at[part, k])
                for k, (rho, buf) in enumerate(((rho_re, in_re), (rho_im, in_im)))]

    def load(c):
        rows = pl.ds(c * GROUP, GROUP)
        return [pltpu.make_async_copy(rho.at[rows], buf.at[rows], in_sem.at[c, k])
                for k, (rho, buf) in enumerate(((rho_re, in_re), (rho_im, in_im)))]

    small = [pltpu.make_async_copy(src, dst, small_sem.at[k]) for k, (src, dst) in enumerate(
        ((w_first, v_first), (w_z, v_z), (w_back, v_back), (w_last, v_last), (g_re, gv_re), (g_im, gv_im)))]

    small[0].start()
    for part in range(BLOCK // QUARTER):
        for copy in load_part(part):
            copy.start()
    lane = lax.broadcasted_iota(jnp.int32, (8, 128), 1)
    real = real_rows()

    def swap(a, b):
        return jnp.where(real, a, pltpu.roll(b, PAIR, 0)), jnp.where(real, pltpu.roll(a, 8 - PAIR, 0), b)

    def target(phase, u, slot):
        return last.at[u, slot] if phase == 3 else got.at[phase, u, slot]

    def remote(phase, u, d, part=None):
        name = axis[phase]
        to = lax.rem(me[name] + d, SIDE)
        src, dst = sent.at[phase, u, to], target(phase, u, me[name])
        if part is not None:
            src, dst = src.at[part], dst.at[part]
        return pltpu.make_async_remote_copy(
            src_ref=src, dst_ref=dst, send_sem=send_sem.at[phase, u, d - 1], recv_sem=recv_sem.at[phase, u, d - 1],
            device_id={name: to}, device_id_type=MESH)

    def own(phase, u):
        mine = me[axis[phase]]
        return pltpu.make_async_copy(sent.at[phase, u, mine], target(phase, u, mine), own_sem.at[phase, u])

    def half_ends(phase, h, to, mine):
        if phase == 0:
            return sent.at[0, 0, to], half_got.at[0, h, mine]
        if phase == 1:
            return half_sent.at[0, h, to], got.at[1, 0, mine]
        if phase == 2:
            return sent.at[2, units - 1, to], half_got.at[1, h, mine]
        return half_sent.at[1, h, to], last.at[units - 1, mine]

    def remote_half(phase, h, d, part=None):
        name = axis[phase]
        to = lax.rem(me[name] + d, SIDE)
        where = pl.ds(0, BLOCK) if part is None else part, pl.ds(QUAD * h, QUAD)
        src, dst = half_ends(phase, h, to, me[name])
        return pltpu.make_async_remote_copy(
            src_ref=src.at[where], dst_ref=dst.at[where],
            send_sem=half_send_sem.at[phase, h, d - 1], recv_sem=half_recv_sem.at[phase, h, d - 1],
            device_id={name: to}, device_id_type=MESH)

    def own_half(phase, h):
        mine = me[axis[phase]]
        where = pl.ds(0, BLOCK), pl.ds(QUAD * h, QUAD)
        src, dst = half_ends(phase, h, mine, mine)
        return pltpu.make_async_copy(src.at[where], dst.at[where], half_own_sem.at[phase, h])

    def send_half(phase, h):
        for d in (2, 1, 3) if axis[phase] == "pz" else (1, 3, 2):
            remote_half(phase, h, d).start()
        own_half(phase, h).start()

    def arrive_half(phase, h):
        for d in range(1, SIDE):
            remote_half(phase, h, d).wait_recv()
        own_half(phase, h).wait()

    def half_y_stage(phase, sign):
        def one(h, carry):
            for k in range(2):
                @pl.when(h == k)
                def _():
                    arrive_half(phase, k)

            dft64(half_got.at[phase // 2, h], half_sent.at[phase // 2, h], tmp, sign)
            for k in range(2):
                @pl.when(h == k)
                def _():
                    send_half(phase + 1, k)

            return carry

        lax.fori_loop(0, 2, one, 0)

    def send(phase, u):
        for d in (2, 1, 3) if axis[phase] == "pz" else (1, 3, 2):
            remote(phase, u, d).start()
        own(phase, u).start()

    def arrive(phase, u):
        for d in range(1, SIDE):
            remote(phase, u, d).wait_recv()
        own(phase, u).wait()

    def x_rows(c, part):
        def one(i, carry):
            rows = pl.ds(c * GROUP, GROUP)
            start = part * QUARTER + i * X_STEP
            both = []
            for k in range(X_STEP):
                re = in_re[rows, start + k].reshape(GROUP * BLOCK, GRID)
                im = in_im[rows, start + k].reshape(GROUP * BLOCK, GRID)
                both.append(jnp.concatenate([re, im], axis=1))
            out = lax.dot_general(v_first[...], jnp.concatenate(both, axis=0), (((1,), (1,)), ((), ())),
                                  precision=HIGHEST, preferred_element_type=jnp.float32)
            out = out.reshape(QUAD, SIDE, 2 * QUAD, X_STEP * 128)
            for k in range(X_STEP):
                for q in range(QUAD):
                    for j in range(SIDE):
                        sent[0, QUAD * c + q, j, start + k] = out[q, j, :, k * 128:(k + 1) * 128]
            return carry

        lax.fori_loop(0, QUARTER // X_STEP, one, 0)

    def send_part(part):
        for d in (1, 3, 2):
            remote_half(0, 0, d, pl.ds(part * QUARTER, QUARTER)).start()

    def first_stage(c):
        lax.fori_loop(0, BLOCK // QUARTER, lambda part, k: (x_rows(c, part), k)[1], 0)
        for q in range(QUAD):
            send(0, QUAD * c + q)

    def opening():
        def quarter(part, carry):
            for copy in load_part(part):
                copy.wait()
            x_rows(0, part)

            @pl.when(part == 1)
            def _():
                pl.semaphore_wait(barrier, 2 * (SIDE - 1))
                send_part(0)

            @pl.when(part >= 1)
            def _():
                send_part(part)

            return carry

        lax.fori_loop(0, BLOCK // QUARTER, quarter, 0)
        own_half(0, 0).start()
        send_half(0, 1)
        for q in range(1, QUAD):
            send(0, q)

    def y_stage(u):
        @pl.when(u > 0)
        def _():
            arrive(0, u)
            dft64(got.at[0, u], sent.at[1, u], tmp, -1)
            send(1, u)

    def z_stage(u):
        c, h = lax.div(u, 2), lax.rem(u, 2)
        @pl.when(u == 0)
        def _():
            for h in range(2):
                arrive_half(1, h)

        @pl.when(u > 0)
        def _():
            arrive(1, 2 * u)

        arrive(1, 2 * u + 1)

        def one(step, carry):
            rows = []
            for i in range(Z_STEP):
                ky = step * Z_STEP + i
                parts = [swap(got[1, 2 * u, s, ky], got[1, 2 * u + 1, s, ky]) for s in range(SIDE)]
                rows += block_transpose([part[k] for k in range(2) for part in parts], lane)
            x = jnp.dot(jnp.concatenate(rows, axis=0), v_z[...], precision=HIGHEST,
                        preferred_element_type=jnp.float32)
            x = x.reshape(Z_STEP, GROUP, HALF, 128)
            scaled = []
            for i in range(Z_STEP):
                ky = step * Z_STEP + i
                a, b = ga[h, ky], gb[h, ky]
                for f in range(GROUP):
                    v = x[i, f]
                    v = v * a + pltpu.roll(v, GRID, 1) * b
                    place = pl.ds(h * (HALF * BLOCK) + ky, HALF, stride=BLOCK)
                    hat_re[c * GROUP + f, place, :] = v[:, :GRID]
                    hat_im[c * GROUP + f, place, :] = pltpu.roll(v, GRID, 1)[:, :GRID]
                    scaled.append(v)
            x = jnp.dot(jnp.concatenate(scaled, axis=0), v_back[...], precision=HIGHEST,
                        preferred_element_type=jnp.float32)
            x = x.reshape(Z_STEP, GROUP, HALF, 128)
            for i in range(Z_STEP):
                ky = step * Z_STEP + i
                out = block_transpose([x[i, f] for f in range(GROUP)], lane)
                for s in range(SIDE):
                    sent[2, 2 * u, s, ky], sent[2, 2 * u + 1, s, ky] = swap(out[s], out[SIDE + s])
            return carry

        lax.fori_loop(0, BLOCK // Z_STEP, one, 0)
        send(2, 2 * u)

        @pl.when(2 * u + 2 < units)
        def _():
            send(2, 2 * u + 1)

        @pl.when(2 * u + 2 == units)
        def _():
            for h in range(2):
                send_half(2, h)

    def back_y_stage(u):
        @pl.when(u + 1 < units)
        def _():
            arrive(2, u)
            dft64(got.at[2, u], sent.at[3, u], tmp, 1)
            send(3, u)

    def last_stage(c):
        for q in range(QUAD):
            arrive(3, QUAD * c + q)
        back_x(last, QUAD * c, v_last, phi_re, phi_im, c * GROUP)

    for c in range(1, chunks):
        for copy in load(c):
            copy.start()
    for copy in small[1:]:
        copy.start()
    small[0].wait()
    opening()
    for copy in small[1:]:
        copy.wait()

    def spread(ky, carry):
        for h in range(2):
            pick = pl.ds(h * HALF * BLOCK + ky, HALF, stride=BLOCK)
            re, im = gv_re[pick, :], gv_im[pick, :]
            ga[h, ky] = jnp.concatenate([re, re], axis=1)
            gb[h, ky] = jnp.concatenate([-im, im], axis=1)
        return carry

    lax.fori_loop(0, BLOCK, spread, 0)
    half_y_stage(0, -1)

    pairs = units // 2

    def step(t, carry):
        @pl.when(t < pairs)
        def _():
            lax.fori_loop(2 * t, 2 * t + 2, lambda u, k: (y_stage(u), k)[1], 0)

        @pl.when((lax.rem(t, 2) == 0) & (t // 2 + 1 < chunks))
        def _():
            c = lax.div(t, 2) + 1
            for copy in load(c):
                copy.wait()
            first_stage(c)

        @pl.when((t >= 3) & (t < pairs + 3))
        def _():
            z_stage(t - 3)

        @pl.when(t >= LAG)
        def _():
            lax.fori_loop(2 * (t - LAG), 2 * (t - LAG) + 2, lambda u, k: (back_y_stage(u), k)[1], 0)

        @pl.when((t >= LAG + 2) & (lax.rem(t - LAG, 2) == 0))
        def _():
            last_stage(lax.div(t - LAG, 2) - 1)

        return carry

    lax.fori_loop(0, pairs + LAG, step, 0)

    def sent_all(phase, first, end):
        def one(u, carry):
            for d in range(1, SIDE):
                remote(phase, u, d).wait_send()
            return carry

        lax.fori_loop(first, end, one, 0)

    half_y_stage(2, 1)
    for phase, first, end in ((0, 1, units), (1, 1, units), (2, 0, units - 1), (3, 0, units - 2)):
        sent_all(phase, first, end)
    for q in range(QUAD - 1):
        arrive(3, units - QUAD + q)
    for h in range(2):
        arrive_half(3, h)
    sent_all(3, units - 2, units - 1)
    for phase in range(4):
        for h in range(2):
            for d in range(1, SIDE):
                remote_half(phase, h, d).wait_send()


def back_x(src, unit, table, out_re, out_im, start):
    def one(i, carry):
        x = [jnp.concatenate([src[unit + q, j, i * X_STEP + k] for q in range(QUAD) for j in range(SIDE)], axis=0)
             for k in range(X_STEP)]
        out = lax.dot_general(jnp.concatenate(x, axis=1), table[...], (((0,), (0,)), ((), ())), precision=HIGHEST,
                              preferred_element_type=jnp.float32)
        where = pl.ds(start, GROUP)
        for k in range(X_STEP):
            place = pl.ds(pl.multiple_of((i * X_STEP + k) * BLOCK, BLOCK), BLOCK)
            part = out[k * 128:(k + 1) * 128]
            out_re[where, place, :] = part[:, :GRID].reshape(GROUP, BLOCK, GRID)
            out_im[where, place, :] = pltpu.roll(part, GRID, 1)[:, :GRID].reshape(GROUP, BLOCK, GRID)
        return carry

    lax.fori_loop(0, BLOCK // X_STEP, one, 0)


def write_out(phi_re, phi_im, hat_re, hat_im, last, table, out_phi_re, out_phi_im, out_hat_re, out_hat_im,
              re, im, sem):
    done = phi_re.shape[0]
    copies = [pltpu.make_async_copy(src, dst, sem.at[k]) for k, (src, dst) in enumerate((
        (hat_re, out_hat_re), (hat_im, out_hat_im), (phi_re, out_phi_re.at[pl.ds(0, done)]),
        (phi_im, out_phi_im.at[pl.ds(0, done)])))]
    for copy in copies:
        copy.start()
    back_x(last, last.shape[0] - QUAD, table, re, im, 0)
    for k, (src, dst) in enumerate(((re, out_phi_re), (im, out_phi_im))):
        copies.append(pltpu.make_async_copy(src, dst.at[pl.ds(done, GROUP)], sem.at[4 + k]))
        copies[-1].start()
    for copy in copies:
        copy.wait()


QUARTER = 4
LAG = 6
X_STEP = 4
Z_STEP = 4


def solve(rho_re, rho_im, g_re, g_im):
    fields = rho_re.shape[0]
    chunks = fields // GROUP
    units = QUAD * chunks
    f32 = jnp.float32
    vmem = pl.BlockSpec(memory_space=pltpu.VMEM)
    anywhere = pl.BlockSpec(memory_space=pl.ANY)
    weights = [jnp.asarray(t) for t in tables()]
    dma = pltpu.SemaphoreType.DMA
    flat = BLOCK * BLOCK
    square = pltpu.VMEM((128, 128), f32)
    held = pl.pallas_call(
        kernel,
        out_shape=[pltpu.VMEM((fields - GROUP, flat, GRID), f32)] * 2 + [pltpu.VMEM((fields, flat, GRID), f32)] * 2
        + [pltpu.VMEM((units, SIDE, BLOCK, 2 * QUAD, 128), f32)],
        in_specs=[anywhere] * 8,
        out_specs=[vmem] * 5,
        scratch_shapes=[
            pltpu.VMEM((fields, BLOCK, BLOCK, GRID), f32),
            pltpu.VMEM((fields, BLOCK, BLOCK, GRID), f32),
            pltpu.VMEM((4, units, SIDE, BLOCK, 2 * QUAD, 128), f32),
            pltpu.VMEM((3, units, SIDE, BLOCK, 2 * QUAD, 128), f32),
            pltpu.VMEM((2, 2, SIDE, BLOCK, 2 * QUAD, 128), f32),
            pltpu.VMEM((2, 2, SIDE, BLOCK, 2 * QUAD, 128), f32),
            pltpu.VMEM((8, 8, 2 * QUAD, 128), f32),
            pltpu.VMEM((flat, GRID), f32),
            pltpu.VMEM((flat, GRID), f32),
            pltpu.VMEM((2, BLOCK, HALF, 128), f32),
            pltpu.VMEM((2, BLOCK, HALF, 128), f32),
            square, square, square, square,
            dma((BLOCK // QUARTER, 2)), dma((chunks, 2)), dma((6,)), dma((4, units)),
            dma((4, units, SIDE - 1)), dma((4, units, SIDE - 1)),
            dma((4, 2)), dma((4, 2, SIDE - 1)), dma((4, 2, SIDE - 1)),
        ],
        compiler_params=pltpu.CompilerParams(collective_id=0, has_side_effects=True, vmem_limit_bytes=41 * 2**20),
        name="spectral_solve",
    )(jnp.transpose(rho_re, (0, 2, 3, 1)), jnp.transpose(rho_im, (0, 2, 3, 1)),
      g_re.reshape(flat, GRID), g_im.reshape(flat, GRID), *weights)
    held = [pltpu.with_memory_space_constraint(x, pltpu.VMEM) for x in held]
    phi_re, phi_im, hat_re, hat_im = pl.pallas_call(
        write_out,
        out_shape=[jax.ShapeDtypeStruct((fields, flat, GRID), f32)] * 4,
        in_specs=[vmem] * 6,
        out_specs=[anywhere] * 4,
        scratch_shapes=[pltpu.VMEM((GROUP, flat, GRID), f32), pltpu.VMEM((GROUP, flat, GRID), f32), dma((6,))],
        compiler_params=pltpu.CompilerParams(vmem_limit_bytes=6 * 2**20),
        name="write_out",
    )(*held, weights[3])
    shape = (fields, BLOCK, BLOCK, GRID)
    phi_re = jnp.transpose(phi_re.reshape(shape), (0, 3, 1, 2))
    phi_im = jnp.transpose(phi_im.reshape(shape), (0, 3, 1, 2))
    return phi_re, phi_im, hat_re.reshape(shape), hat_im.reshape(shape)


def solution(mesh):
    space_layout = P("dp", None, "py", "pz")
    wave_layout = P("dp", "py", "pz", None)
    green_layout = P("py", "pz", None)
    return jax.shard_map(solve, mesh=mesh,
                         in_specs=(space_layout, space_layout, green_layout, green_layout),
                         out_specs=(space_layout, space_layout, wave_layout, wave_layout),
                         check_vma=False)
```

```python
import jax
import jax.numpy as jnp
import numpy as np
from jax import lax
from jax.experimental import pallas as pl
from jax.experimental.pallas import tpu as pltpu
from jax.sharding import PartitionSpec as P

GRID = 64
SIDE = 4
BLOCK = 16
GROUP = 8
HALF = 8
QUAD = 4
PAIR = 2
HIGHEST = lax.Precision.HIGHEST
MESH = pl.DeviceIdType.MESH


def rotation(left, right, sign):
    angle = 2.0 * np.pi * (np.outer(left, right) % GRID) / GRID
    return np.cos(angle), sign * np.sin(angle)


def dft_matrix(rows_in, rows_out, sign, scale):
    cos, sin = rotation(rows_in, rows_out, sign)
    return np.block([[cos, sin], [-sin, cos]]) * scale


def tables():
    points = np.arange(GRID)
    q, j, h, c, k = np.ix_(range(QUAD), range(SIDE), range(2), range(2), range(PAIR))
    order = (BLOCK * j + HALF * (q // 2) + PAIR * (q % 2) + QUAD * h + k + GRID * c).reshape(-1)
    first = dft_matrix(points, points, -1, 1.0 / 64).T[order]
    last = dft_matrix(points, points, 1, 1.0 / 8)[order]
    along_z = dft_matrix(points, points, -1, 1.0 / 8)
    back_z = dft_matrix(points, points, 1, 1.0 / 64)
    return [np.asarray(t, np.float32) for t in (first, along_z, back_z, last)]


def dft4(x, turn):
    even, odd = x[0] + x[2], x[0] - x[2]
    both, side = x[1] + x[3], turn(x[1] - x[3])
    return [even + both, odd + side, even - both, odd - side]


def dft8(x, turn):
    r = np.float32(np.sqrt(0.5))
    even = [x[i] + x[i + 4] for i in range(4)]
    odd = [x[i] - x[i + 4] for i in range(4)]
    odd = [odd[0], (odd[1] + turn(odd[1])) * r, turn(odd[2]), (turn(odd[3]) - odd[3]) * r]
    even, odd = dft4(even, turn), dft4(odd, turn)
    return [value for pair in zip(even, odd) for value in pair]


def real_rows():
    return (lax.broadcasted_iota(jnp.int32, (8, 128), 0) & PAIR) == 0


def dft64(src, dst, tmp, sign):
    real = real_rows()
    signs = jnp.where(real, np.float32(-sign), np.float32(sign))

    def turn(value):
        return jnp.where(real, pltpu.roll(value, 8 - PAIR, 0), pltpu.roll(value, PAIR, 0)) * signs

    def twiddle(value, power):
        if power == 0:
            return value
        angle = 2 * np.pi * power / GRID
        return value * np.float32(np.cos(angle)) + turn(value) * np.float32(np.sin(angle))

    for b in range(8):
        x = [src[divmod(8 * a + b, BLOCK)] for a in range(8)]
        for k, value in enumerate(dft8(x, turn)):
            tmp[b, k] = twiddle(value, b * k)
    for k in range(8):
        out = dft8([tmp[b, k] for b in range(8)], turn)
        for m, value in enumerate(out):
            dst[divmod(k + 8 * m, BLOCK)] = value


def block_transpose(x, lane):
    x = list(x)
    for bit in range(3):
        shift = BLOCK << bit
        low = (lane & shift) == 0
        for i in range(8):
            if i & (1 << bit) == 0:
                j = i | (1 << bit)
                a, b = x[i], x[j]
                x[i] = jnp.where(low, a, pltpu.roll(b, shift, 1))
                x[j] = jnp.where(low, pltpu.roll(a, 128 - shift, 1), b)
    return x


def kernel(rho_re, rho_im, g_re, g_im, w_first, w_z, w_back, w_last, phi_re, phi_im, hat_re, hat_im, last,
           in_re, in_im, sent, got, half_got, half_sent, tmp, gv_re, gv_im, ga, gb, v_first, v_z, v_back, v_last,
           part_sem, in_sem, small_sem, own_sem, send_sem, recv_sem,
           half_own_sem, half_send_sem, half_recv_sem):
    fields = rho_re.shape[0]
    chunks = fields // GROUP
    units = QUAD * chunks
    axis = ("py", "pz", "pz", "py")
    me = {name: lax.axis_index(name) for name in ("py", "pz")}

    barrier = pltpu.get_barrier_semaphore()
    for name in ("py", "pz"):
        for d in range(1, SIDE):
            pl.semaphore_signal(barrier, inc=1, device_id={name: lax.rem(me[name] + d, SIDE)}, device_id_type=MESH)

    def load_part(part):
        where = pl.ds(0, GROUP), pl.ds(part * QUARTER, QUARTER)
        return [pltpu.make_async_copy(rho.at[where], buf.at[where], part_sem.at[part, k])
                for k, (rho, buf) in enumerate(((rho_re, in_re), (rho_im, in_im)))]

    def load(c):
        rows = pl.ds(c * GROUP, GROUP)
        return [pltpu.make_async_copy(rho.at[rows], buf.at[rows], in_sem.at[c, k])
                for k, (rho, buf) in enumerate(((rho_re, in_re), (rho_im, in_im)))]

    small = [pltpu.make_async_copy(src, dst, small_sem.at[k]) for k, (src, dst) in enumerate(
        ((w_first, v_first), (w_z, v_z), (w_back, v_back), (w_last, v_last), (g_re, gv_re), (g_im, gv_im)))]

    small[0].start()
    for part in range(BLOCK // QUARTER):
        for copy in load_part(part):
            copy.start()
    lane = lax.broadcasted_iota(jnp.int32, (8, 128), 1)
    real = real_rows()

    def swap(a, b):
        return jnp.where(real, a, pltpu.roll(b, PAIR, 0)), jnp.where(real, pltpu.roll(a, 8 - PAIR, 0), b)

    def target(phase, u, slot):
        return last.at[u, slot] if phase == 3 else got.at[phase, u, slot]

    def remote(phase, u, d, part=None):
        name = axis[phase]
        to = lax.rem(me[name] + d, SIDE)
        src, dst = sent.at[phase, u, to], target(phase, u, me[name])
        if part is not None:
            src, dst = src.at[part], dst.at[part]
        return pltpu.make_async_remote_copy(
            src_ref=src, dst_ref=dst, send_sem=send_sem.at[phase, u, d - 1], recv_sem=recv_sem.at[phase, u, d - 1],
            device_id={name: to}, device_id_type=MESH)

    def own(phase, u):
        mine = me[axis[phase]]
        return pltpu.make_async_copy(sent.at[phase, u, mine], target(phase, u, mine), own_sem.at[phase, u])

    def half_ends(phase, h, to, mine):
        if phase == 0:
            return sent.at[0, 0, to], half_got.at[0, h, mine]
        if phase == 1:
            return half_sent.at[0, h, to], got.at[1, 0, mine]
        if phase == 2:
            return sent.at[2, units - 1, to], half_got.at[1, h, mine]
        return half_sent.at[1, h, to], last.at[units - 1, mine]

    def remote_half(phase, h, d, part=None):
        name = axis[phase]
        to = lax.rem(me[name] + d, SIDE)
        where = pl.ds(0, BLOCK) if part is None else part, pl.ds(QUAD * h, QUAD)
        src, dst = half_ends(phase, h, to, me[name])
        return pltpu.make_async_remote_copy(
            src_ref=src.at[where], dst_ref=dst.at[where],
            send_sem=half_send_sem.at[phase, h, d - 1], recv_sem=half_recv_sem.at[phase, h, d - 1],
            device_id={name: to}, device_id_type=MESH)

    def own_half(phase, h):
        mine = me[axis[phase]]
        where = pl.ds(0, BLOCK), pl.ds(QUAD * h, QUAD)
        src, dst = half_ends(phase, h, mine, mine)
        return pltpu.make_async_copy(src.at[where], dst.at[where], half_own_sem.at[phase, h])

    def send_half(phase, h):
        for d in (2, 1, 3) if axis[phase] == "pz" else (1, 3, 2):
            remote_half(phase, h, d).start()
        own_half(phase, h).start()

    def arrive_half(phase, h):
        for d in range(1, SIDE):
            remote_half(phase, h, d).wait_recv()
        own_half(phase, h).wait()

    def half_y_stage(phase, sign):
        def one(h, carry):
            for k in range(2):
                @pl.when(h == k)
                def _():
                    arrive_half(phase, k)

            dft64(half_got.at[phase // 2, h], half_sent.at[phase // 2, h], tmp, sign)
            for k in range(2):
                @pl.when(h == k)
                def _():
                    send_half(phase + 1, k)

            return carry

        lax.fori_loop(0, 2, one, 0)

    def send(phase, u):
        for d in (2, 1, 3) if axis[phase] == "pz" else (1, 3, 2):
            remote(phase, u, d).start()
        own(phase, u).start()

    def arrive(phase, u):
        for d in range(1, SIDE):
            remote(phase, u, d).wait_recv()
        own(phase, u).wait()

    def x_rows(c, part):
        def one(i, carry):
            rows = pl.ds(c * GROUP, GROUP)
            start = part * QUARTER + i * X_STEP
            both = []
            for k in range(X_STEP):
                re = in_re[rows, start + k].reshape(GROUP * BLOCK, GRID)
                im = in_im[rows, start + k].reshape(GROUP * BLOCK, GRID)
                both.append(jnp.concatenate([re, im], axis=1))
            out = lax.dot_general(v_first[...], jnp.concatenate(both, axis=0), (((1,), (1,)), ((), ())),
                                  precision=HIGHEST, preferred_element_type=jnp.float32)
            out = out.reshape(QUAD, SIDE, 2 * QUAD, X_STEP * 128)
            for k in range(X_STEP):
                for q in range(QUAD):
                    for j in range(SIDE):
                        sent[0, QUAD * c + q, j, start + k] = out[q, j, :, k * 128:(k + 1) * 128]
            return carry

        lax.fori_loop(0, QUARTER // X_STEP, one, 0)

    def send_part(part):
        for d in (1, 3, 2):
            remote_half(0, 0, d, pl.ds(part * QUARTER, QUARTER)).start()

    def first_stage(c):
        lax.fori_loop(0, BLOCK // QUARTER, lambda part, k: (x_rows(c, part), k)[1], 0)
        for q in range(QUAD):
            send(0, QUAD * c + q)

    def opening():
        def quarter(part, carry):
            for copy in load_part(part):
                copy.wait()
            x_rows(0, part)

            @pl.when(part == 0)
            def _():
                pl.semaphore_wait(barrier, 2 * (SIDE - 1))

            send_part(part)
            return carry

        lax.fori_loop(0, BLOCK // QUARTER, quarter, 0)
        own_half(0, 0).start()
        send_half(0, 1)
        for q in range(1, QUAD):
            send(0, q)

    def y_stage(u):
        @pl.when(u > 0)
        def _():
            arrive(0, u)
            dft64(got.at[0, u], sent.at[1, u], tmp, -1)
            send(1, u)

    def z_stage(u):
        c, h = lax.div(u, 2), lax.rem(u, 2)
        @pl.when(u == 0)
        def _():
            for h in range(2):
                arrive_half(1, h)

        @pl.when(u > 0)
        def _():
            arrive(1, 2 * u)

        arrive(1, 2 * u + 1)

        def one(step, carry):
            rows = []
            for i in range(Z_STEP):
                ky = step * Z_STEP + i
                parts = [swap(got[1, 2 * u, s, ky], got[1, 2 * u + 1, s, ky]) for s in range(SIDE)]
                rows += block_transpose([part[k] for k in range(2) for part in parts], lane)
            x = jnp.dot(jnp.concatenate(rows, axis=0), v_z[...], precision=HIGHEST,
                        preferred_element_type=jnp.float32)
            x = x.reshape(Z_STEP, GROUP, HALF, 128)
            scaled = []
            for i in range(Z_STEP):
                ky = step * Z_STEP + i
                a, b = ga[h, ky], gb[h, ky]
                for f in range(GROUP):
                    v = x[i, f]
                    v = v * a + pltpu.roll(v, GRID, 1) * b
                    place = pl.ds(h * (HALF * BLOCK) + ky, HALF, stride=BLOCK)
                    hat_re[c * GROUP + f, place, :] = v[:, :GRID]
                    hat_im[c * GROUP + f, place, :] = pltpu.roll(v, GRID, 1)[:, :GRID]
                    scaled.append(v)
            x = jnp.dot(jnp.concatenate(scaled, axis=0), v_back[...], precision=HIGHEST,
                        preferred_element_type=jnp.float32)
            x = x.reshape(Z_STEP, GROUP, HALF, 128)
            for i in range(Z_STEP):
                ky = step * Z_STEP + i
                out = block_transpose([x[i, f] for f in range(GROUP)], lane)
                for s in range(SIDE):
                    sent[2, 2 * u, s, ky], sent[2, 2 * u + 1, s, ky] = swap(out[s], out[SIDE + s])
            return carry

        lax.fori_loop(0, BLOCK // Z_STEP, one, 0)
        send(2, 2 * u)

        @pl.when(2 * u + 2 < units)
        def _():
            send(2, 2 * u + 1)

        @pl.when(2 * u + 2 == units)
        def _():
            for h in range(2):
                send_half(2, h)

    def back_y_stage(u):
        @pl.when(u + 1 < units)
        def _():
            arrive(2, u)
            dft64(got.at[2, u], sent.at[3, u], tmp, 1)
            send(3, u)

    def last_stage(c):
        for q in range(QUAD):
            arrive(3, QUAD * c + q)
        back_x(last, QUAD * c, v_last, phi_re, phi_im, c * GROUP)

    for c in range(1, chunks):
        for copy in load(c):
            copy.start()
    for copy in small[1:]:
        copy.start()
    small[0].wait()
    opening()
    for copy in small[1:]:
        copy.wait()

    def spread(ky, carry):
        for h in range(2):
            pick = pl.ds(h * HALF * BLOCK + ky, HALF, stride=BLOCK)
            re, im = gv_re[pick, :], gv_im[pick, :]
            ga[h, ky] = jnp.concatenate([re, re], axis=1)
            gb[h, ky] = jnp.concatenate([-im, im], axis=1)
        return carry

    lax.fori_loop(0, BLOCK, spread, 0)
    half_y_stage(0, -1)

    pairs = units // 2

    def step(t, carry):
        @pl.when(t < pairs)
        def _():
            lax.fori_loop(2 * t, 2 * t + 2, lambda u, k: (y_stage(u), k)[1], 0)

        @pl.when((lax.rem(t, 2) == 0) & (t // 2 + 1 < chunks))
        def _():
            c = lax.div(t, 2) + 1
            for copy in load(c):
                copy.wait()
            first_stage(c)

        @pl.when((t >= 7) & (t < pairs + 7))
        def _():
            z_stage(t - 7)

        @pl.when(t >= LAG)
        def _():
            lax.fori_loop(2 * (t - LAG), 2 * (t - LAG) + 2, lambda u, k: (back_y_stage(u), k)[1], 0)

        @pl.when((t >= LAG + 2) & (lax.rem(t - LAG, 2) == 0))
        def _():
            last_stage(lax.div(t - LAG, 2) - 1)

        return carry

    lax.fori_loop(0, pairs + LAG, step, 0)

    def sent_all(phase, first, end):
        def one(u, carry):
            for d in range(1, SIDE):
                remote(phase, u, d).wait_send()
            return carry

        lax.fori_loop(first, end, one, 0)

    half_y_stage(2, 1)
    for phase, first, end in ((0, 1, units), (1, 1, units), (2, 0, units - 1), (3, 0, units - 2)):
        sent_all(phase, first, end)
    for q in range(QUAD - 1):
        arrive(3, units - QUAD + q)
    for h in range(2):
        arrive_half(3, h)
    sent_all(3, units - 2, units - 1)
    for phase in range(4):
        for h in range(2):
            for d in range(1, SIDE):
                remote_half(phase, h, d).wait_send()


def back_x(src, unit, table, out_re, out_im, start):
    def one(i, carry):
        x = [jnp.concatenate([src[unit + q, j, i * X_STEP + k] for q in range(QUAD) for j in range(SIDE)], axis=0)
             for k in range(X_STEP)]
        out = lax.dot_general(jnp.concatenate(x, axis=1), table[...], (((0,), (0,)), ((), ())), precision=HIGHEST,
                              preferred_element_type=jnp.float32)
        where = pl.ds(start, GROUP)
        for k in range(X_STEP):
            place = pl.ds(pl.multiple_of((i * X_STEP + k) * BLOCK, BLOCK), BLOCK)
            part = out[k * 128:(k + 1) * 128]
            out_re[where, place, :] = part[:, :GRID].reshape(GROUP, BLOCK, GRID)
            out_im[where, place, :] = pltpu.roll(part, GRID, 1)[:, :GRID].reshape(GROUP, BLOCK, GRID)
        return carry

    lax.fori_loop(0, BLOCK // X_STEP, one, 0)


def write_out(phi_re, phi_im, hat_re, hat_im, last, table, out_phi_re, out_phi_im, out_hat_re, out_hat_im,
              re, im, sem):
    done = phi_re.shape[0]
    copies = [pltpu.make_async_copy(src, dst, sem.at[k]) for k, (src, dst) in enumerate((
        (hat_re, out_hat_re), (hat_im, out_hat_im), (phi_re, out_phi_re.at[pl.ds(0, done)]),
        (phi_im, out_phi_im.at[pl.ds(0, done)])))]
    for copy in copies:
        copy.start()
    back_x(last, last.shape[0] - QUAD, table, re, im, 0)
    for k, (src, dst) in enumerate(((re, out_phi_re), (im, out_phi_im))):
        copies.append(pltpu.make_async_copy(src, dst.at[pl.ds(done, GROUP)], sem.at[4 + k]))
        copies[-1].start()
    for copy in copies:
        copy.wait()


QUARTER = 4
LAG = 13
X_STEP = 4
Z_STEP = 4


def solve(rho_re, rho_im, g_re, g_im):
    fields = rho_re.shape[0]
    chunks = fields // GROUP
    units = QUAD * chunks
    f32 = jnp.float32
    vmem = pl.BlockSpec(memory_space=pltpu.VMEM)
    anywhere = pl.BlockSpec(memory_space=pl.ANY)
    weights = [jnp.asarray(t) for t in tables()]
    dma = pltpu.SemaphoreType.DMA
    flat = BLOCK * BLOCK
    square = pltpu.VMEM((128, 128), f32)
    held = pl.pallas_call(
        kernel,
        out_shape=[pltpu.VMEM((fields - GROUP, flat, GRID), f32)] * 2 + [pltpu.VMEM((fields, flat, GRID), f32)] * 2
        + [pltpu.VMEM((units, SIDE, BLOCK, 2 * QUAD, 128), f32)],
        in_specs=[anywhere] * 8,
        out_specs=[vmem] * 5,
        scratch_shapes=[
            pltpu.VMEM((fields, BLOCK, BLOCK, GRID), f32),
            pltpu.VMEM((fields, BLOCK, BLOCK, GRID), f32),
            pltpu.VMEM((4, units, SIDE, BLOCK, 2 * QUAD, 128), f32),
            pltpu.VMEM((3, units, SIDE, BLOCK, 2 * QUAD, 128), f32),
            pltpu.VMEM((2, 2, SIDE, BLOCK, 2 * QUAD, 128), f32),
            pltpu.VMEM((2, 2, SIDE, BLOCK, 2 * QUAD, 128), f32),
            pltpu.VMEM((8, 8, 2 * QUAD, 128), f32),
            pltpu.VMEM((flat, GRID), f32),
            pltpu.VMEM((flat, GRID), f32),
            pltpu.VMEM((2, BLOCK, HALF, 128), f32),
            pltpu.VMEM((2, BLOCK, HALF, 128), f32),
            square, square, square, square,
            dma((BLOCK // QUARTER, 2)), dma((chunks, 2)), dma((6,)), dma((4, units)),
            dma((4, units, SIDE - 1)), dma((4, units, SIDE - 1)),
            dma((4, 2)), dma((4, 2, SIDE - 1)), dma((4, 2, SIDE - 1)),
        ],
        compiler_params=pltpu.CompilerParams(collective_id=0, has_side_effects=True, vmem_limit_bytes=41 * 2**20),
        name="spectral_solve",
    )(jnp.transpose(rho_re, (0, 2, 3, 1)), jnp.transpose(rho_im, (0, 2, 3, 1)),
      g_re.reshape(flat, GRID), g_im.reshape(flat, GRID), *weights)
    held = [pltpu.with_memory_space_constraint(x, pltpu.VMEM) for x in held]
    phi_re, phi_im, hat_re, hat_im = pl.pallas_call(
        write_out,
        out_shape=[jax.ShapeDtypeStruct((fields, flat, GRID), f32)] * 4,
        in_specs=[vmem] * 6,
        out_specs=[anywhere] * 4,
        scratch_shapes=[pltpu.VMEM((GROUP, flat, GRID), f32), pltpu.VMEM((GROUP, flat, GRID), f32), dma((6,))],
        compiler_params=pltpu.CompilerParams(vmem_limit_bytes=6 * 2**20),
        name="write_out",
    )(*held, weights[3])
    shape = (fields, BLOCK, BLOCK, GRID)
    phi_re = jnp.transpose(phi_re.reshape(shape), (0, 3, 1, 2))
    phi_im = jnp.transpose(phi_im.reshape(shape), (0, 3, 1, 2))
    return phi_re, phi_im, hat_re.reshape(shape), hat_im.reshape(shape)


def solution(mesh):
    space_layout = P("dp", None, "py", "pz")
    wave_layout = P("dp", "py", "pz", None)
    green_layout = P("py", "pz", None)
    return jax.shard_map(solve, mesh=mesh,
                         in_specs=(space_layout, space_layout, green_layout, green_layout),
                         out_specs=(space_layout, space_layout, wave_layout, wave_layout),
                         check_vma=False)
```
